256 devices in a mesh: row: 32 (over z, y), dep: 8 (over x, core).
Axes of the slice: x: 4, y: 4, z: 8, core: 2. Of those that a mesh axis runs over, the one named last changes fastest.
Arguments:
- x_vol: bfloat16 [2, 16, 512, 32, 128], P(None, 'dep', 'row')
- w_conv1: bfloat16 [3, 3, 3, 128, 128], replicated
- w_conv2: bfloat16 [3, 3, 3, 128, 128], replicated
- g_out: bfloat16 [2, 16, 512, 32, 128], P(None, 'dep', 'row')
Outputs:
- output 1: bfloat16 [2, 16, 512, 32, 128], P(None, 'dep', 'row')
- output 2: bfloat16 [2, 16, 512, 32, 128], P(None, 'dep', 'row')
- output 3: float32 [3, 3, 3, 128, 128], replicated
- output 4: float32 [3, 3, 3, 128, 128], replicated
All inputs are finite; a program needn't handle non-finite values.
Results may differ from the reference program's by a relative error of at most 0.00921345.
Values are sent between devices in bfloat16 or wider.
A program may use at most 768 MiB of HBM per device.

```python
import jax
import jax.numpy as jnp
from jax import lax

BATCH_SIZE = 2
VOL_DEPTH = 16
VOL_ROWS = 512
VOL_WIDTH = 32
CHANNELS = 128


def setup_inputs(seed: int = 0) -> dict:
    root_key = jax.random.key(seed)
    key_x, key_w1, key_w2, key_g = jax.random.split(root_key, 4)
    vol_shape = (BATCH_SIZE, VOL_DEPTH, VOL_ROWS, VOL_WIDTH, CHANNELS)
    kern_shape = (3, 3, 3, CHANNELS, CHANNELS)
    fan_scale = (27 * CHANNELS) ** -0.5
    x_vol = jax.random.normal(key_x, vol_shape, jnp.float32).astype(jnp.bfloat16)
    w_conv1 = (fan_scale * jax.random.normal(key_w1, kern_shape, jnp.float32)).astype(jnp.bfloat16)
    w_conv2 = (1.5 * fan_scale * jax.random.normal(key_w2, kern_shape, jnp.float32)).astype(jnp.bfloat16)
    g_out = jax.random.normal(key_g, vol_shape, jnp.float32).astype(jnp.bfloat16)
    return {'x_vol': x_vol, 'w_conv1': w_conv1, 'w_conv2': w_conv2, 'g_out': g_out}


def conv_same(volume, kernel):
    return lax.conv_general_dilated(volume, kernel, (1, 1, 1), 'SAME', dimension_numbers=('NDHWC', 'DHWIO', 'NDHWC'))


def gelu_tanh(values):
    return jax.nn.gelu(values, approximate=True)


def reference(x_vol, w_conv1, w_conv2, g_out):
    x_f32 = x_vol.astype(jnp.float32)
    g_f32 = g_out.astype(jnp.float32)
    pre_f32, conv1_back = jax.vjp(conv_same, x_f32, w_conv1.astype(jnp.float32))
    pre_act = pre_f32.astype(jnp.bfloat16)
    gelu_f32, gelu_back = jax.vjp(gelu_tanh, pre_act.astype(jnp.float32))
    gelu_bf = gelu_f32.astype(jnp.bfloat16)
    out_f32, conv2_back = jax.vjp(conv_same, gelu_bf.astype(jnp.float32), w_conv2.astype(jnp.float32))
    y_out = (out_f32 + x_f32).astype(jnp.bfloat16)
    dgelu_f32, dw_conv2 = conv2_back(g_f32)
    dpre_bf = gelu_back(dgelu_f32)[0].astype(jnp.bfloat16)
    dx_f32, dw_conv1 = conv1_back(dpre_bf.astype(jnp.float32))
    dx_vol = (dx_f32 + g_f32).astype(jnp.bfloat16)
    return (y_out, dx_vol, dw_conv1, dw_conv2)
```

```python
import functools

import jax
import jax.numpy as jnp
from jax import lax
from jax.experimental import pallas as pl
from jax.experimental.pallas import tpu as pltpu
from jax.sharding import PartitionSpec as P

MESH = pl.DeviceIdType.MESH
F32 = jnp.float32
BF16 = jnp.bfloat16

NB, ND, NR, NW, NC = 2, 2, 16, 32, 128
TAPS = 27
ROWS = TAPS * NC
HALF = ROWS // 2
GRP = HALF // 2
NEIGH = ((0, 1), (0, -1), (1, 0), (-1, 0), (1, 1), (1, -1), (-1, 1), (-1, -1))


def kernel(nx, ny, nz, x_hbm, w1_hbm, w2_hbm, g_hbm,
           y_hbm, dx_hbm, dw1_hbm, dw2_hbm,
           xe, ge, ze, ae, xc, gc, zc, ac,
           w1r, w2r, w1f, w2f, w1t, w2t, gp, zt, at,
           part, crecv, hsum, r1, s1, r2, s2, r3, t2, t1, th, yv, dxv,
           in_sem, hs_sem, hr_sem, cs_sem, cr_sem, as_sem, ar_sem, out_sem):
    row, dep = lax.axis_index("row"), lax.axis_index("dep")
    nrow, ndep = nz * ny, nx * 2
    zi, yi = row // ny, row % ny
    xi, ci = dep // 2, dep % 2
    other = 1 - ci

    def x_peer(k):
        return (row, ((xi + k) % nx) * 2 + ci)

    def y_peer(k):
        return (zi * ny + (yi + k) % ny, dep)

    def z_peer(k):
        return (((zi + k) % nz) * ny + yi, dep)

    core_peer = (row, xi * 2 + other)

    def halo_peer(dr, dd):
        return ((row + dr + nrow) % nrow, (dep + dd + ndep) % ndep)

    cx = pltpu.make_async_copy(x_hbm, xe.at[:, pl.ds(1, 2), pl.ds(1, NR)], in_sem.at[0])
    cg = pltpu.make_async_copy(g_hbm, ge.at[:, pl.ds(1, 2), pl.ds(1, NR)], in_sem.at[1])
    cw = [
        pltpu.make_async_copy(w2_hbm, w2r, in_sem.at[2]),
        pltpu.make_async_copy(w1_hbm, w1r, in_sem.at[3]),
        pltpu.make_async_copy(w1_hbm, w1f.at[pl.ds(0, ROWS), pl.ds(0, NC)], in_sem.at[4]),
        pltpu.make_async_copy(w1_hbm, w1f.at[pl.ds(1152, ROWS), pl.ds(NC, NC)], in_sem.at[5]),
        pltpu.make_async_copy(w2_hbm, w2f.at[pl.ds(0, ROWS), pl.ds(0, NC)], in_sem.at[6]),
        pltpu.make_async_copy(w2_hbm, w2f.at[pl.ds(1152, ROWS), pl.ds(NC, NC)], in_sem.at[7]),
    ]
    cx.start()
    cg.start()
    for c in cw:
        c.start()

    partners = [halo_peer(a, b) for a, b in NEIGH]
    partners += [x_peer(k) for k in range(1, nx)]
    partners += [y_peer(k) for k in range(1, ny)]
    partners += [z_peer(k) for k in range(1, nz)]
    barrier = pltpu.get_barrier_semaphore()
    for p in partners:
        pl.semaphore_signal(barrier, inc=1, device_id=p, device_id_type=MESH)
    pl.semaphore_wait(barrier, len(partners))

    def halo_copies(slot, ext):
        out = []
        for k, (dr, dd) in enumerate(NEIGH):
            se, de = {1: (pl.ds(2, 1), pl.ds(0, 1)), -1: (pl.ds(1, 1), pl.ds(3, 1)),
                      0: (pl.ds(1, 2), pl.ds(1, 2))}[dd]
            sr, tr = {1: (pl.ds(NR, 1), pl.ds(0, 1)), -1: (pl.ds(1, 1), pl.ds(NR + 1, 1)),
                      0: (pl.ds(1, NR), pl.ds(1, NR))}[dr]
            out.append(pltpu.make_async_remote_copy(
                src_ref=ext.at[:, se, sr], dst_ref=ext.at[:, de, tr],
                send_sem=hs_sem.at[slot, k], recv_sem=hr_sem.at[slot, k],
                device_id=halo_peer(dr, dd), device_id_type=MESH))
        return out

    hx, hg, hz, ha = (halo_copies(i, e) for i, e in enumerate((xe, ge, ze, ae)))
    pending = []

    def start(copies):
        for c in copies:
            c.start()
            pending.append(c)

    def recv(copies):
        for c in copies:
            c.wait_recv()

    cx.wait()
    start(hx)
    cg.wait()
    start(hg)

    w1f[pl.ds(ROWS, 1152), pl.ds(0, NC)] = jnp.zeros((1152, NC), BF16)
    w1f[pl.ds(0, 1152), pl.ds(NC, NC)] = jnp.zeros((1152, NC), BF16)
    w2f[pl.ds(ROWS, 1152), pl.ds(0, NC)] = jnp.zeros((1152, NC), BF16)
    w2f[pl.ds(0, 1152), pl.ds(NC, NC)] = jnp.zeros((1152, NC), BF16)
    w1t[pl.ds(ROWS, 1152), pl.ds(0, NC)] = jnp.zeros((1152, NC), BF16)
    w1t[pl.ds(0, 1152), pl.ds(NC, NC)] = jnp.zeros((1152, NC), BF16)
    w2t[pl.ds(ROWS, 1152), pl.ds(0, NC)] = jnp.zeros((1152, NC), BF16)
    w2t[pl.ds(0, 1152), pl.ds(NC, NC)] = jnp.zeros((1152, NC), BF16)
    for c in cw:
        c.wait()

    def flip(raw, out):
        for u in range(TAPS):
            block = raw[pl.ds((TAPS - 1 - u) * NC, NC), :].T
            out[pl.ds(u * NC, NC), pl.ds(0, NC)] = block
            out[pl.ds(1152 + u * NC, NC), pl.ds(NC, NC)] = block

    flip(w2r, w2t)
    flip(w1r, w1t)

    def widen(vals, store):
        v = vals.astype(F32)
        col = lax.broadcasted_iota(jnp.int32, v.shape, 1)
        left = jnp.where(col == 0, 0.0, pltpu.roll(v, 1, 1))
        right = jnp.where(col == NW - 1, 0.0, pltpu.roll(v, NW - 1, 1))
        store(0, left.astype(BF16))
        store(1, vals)
        store(2, right.astype(BF16))

    def widen_part(ext, out, b, e, r0, nr, keep):
        vals = ext[b, e, pl.ds(r0, nr)]
        if keep is not None:
            vals = jnp.where(keep, vals, jnp.zeros_like(vals))

        def store(j, piece):
            out[b, e, pl.ds(r0, nr), :, pl.ds(j * NC, NC)] = piece

        widen(vals, store)

    def widen_local(ext, out):
        for b in range(NB):
            for e in (1, 2):
                for r0 in (1, 9):
                    widen_part(ext, out, b, e, r0, 8, None)

    def both(a, b):
        return a if b is None else (b if a is None else jnp.logical_and(a, b))

    def widen_halo(ext, out):
        for b in range(NB):
            for e in range(4):
                ek = {0: dep > 0, 3: dep < ndep - 1}.get(e)
                widen_part(ext, out, b, e, 0, 1, both(ek, row > 0))
                widen_part(ext, out, b, e, NR + 1, 1, both(ek, row < nrow - 1))
                if ek is not None:
                    for r0 in (1, 9):
                        widen_part(ext, out, b, e, r0, 8, ek)

    def conv(src, wts, finish):
        for b in range(NB):
            for r0 in (0, 8):
                lhs = jnp.concatenate(
                    [src[b, e, pl.ds(r0 + dr, 8)].reshape(8 * NW, 3 * NC)
                     for e in range(4) for dr in range(3)], axis=1)
                acc = jnp.dot(lhs, wts[...], preferred_element_type=F32)
                for d in range(ND):
                    finish(b, d, r0, acc[:, d * NC:(d + 1) * NC])

    def put(ref, b, d, r0, vals):
        ref[b, d, pl.ds(r0, 8)] = vals.reshape(8, NW, NC)

    def fin_a(b, d, r0, acc):
        a = acc.astype(BF16).astype(F32)
        c0, c1 = 0.7978845608028654, 0.044715
        sq = a * a
        th_ = jnp.tanh(c0 * (a + c1 * (sq * a)))
        cdf = 0.5 * (1.0 + th_)
        z = (a * cdf).astype(BF16)
        slope = cdf + (0.5 * a) * (1.0 - th_ * th_) * (c0 * (1.0 + (3.0 * c1) * sq))
        gp[b, d, pl.ds(r0 * NW, 8 * NW)] = slope
        put(ze, b, d + 1, r0 + 1, z)
        zt[:, pl.ds((d * NB + b) * 512 + r0 * NW, 8 * NW)] = z.T

    def fin_da(b, d, r0, acc):
        da = (acc * gp[b, d, pl.ds(r0 * NW, 8 * NW)]).astype(BF16)
        put(ae, b, d + 1, r0 + 1, da)
        at[:, pl.ds((d * NB + b) * 512 + r0 * NW, 8 * NW)] = da.T

    def fin_add(base, out):
        def fin(b, d, r0, acc):
            res = base[b, d + 1, pl.ds(r0 + 1, 8)].reshape(8 * NW, NC).astype(F32)
            put(out, b, d, r0, (acc + res).astype(BF16))
        return fin

    def tap_rhs(src, u):
        ud, dr, dw = u // 9, (u // 3) % 3, u % 3
        return jnp.concatenate(
            [src[b, d + ud, pl.ds(dr, NR), :, pl.ds(dw * NC, NC)].reshape(NR * NW, NC)
             for d in range(ND) for b in range(NB)], axis=0)

    def wgrad(lhs_t, src, j, flipped):
        lhs = lhs_t[...]
        for u in range(0, TAPS, 2):
            pair = [t for t in (u, u + 1) if t < TAPS]
            rhs = jnp.concatenate([tap_rhs(src, t) for t in pair], axis=1)
            out = jnp.dot(lhs, rhs, preferred_element_type=F32)
            for n, t in enumerate(pair):
                block = out[:, n * NC:(n + 1) * NC]
                if flipped:
                    part[j, pl.ds((TAPS - 1 - t) * NC, NC), :] = block
                else:
                    part[j, pl.ds(t * NC, NC), :] = block.T

    def rcopy(src, dst, ssem, rsem, peer):
        return pltpu.make_async_remote_copy(src_ref=src, dst_ref=dst, send_sem=ssem,
                                            recv_sem=rsem, device_id=peer, device_id_type=MESH)

    def ds8(base, size):
        return pl.ds(pl.multiple_of(base, 8), size)

    def ring(g, stage):
        order = ((x_peer, xi, nx), (y_peer, yi, ny))
        return order[(g + stage) % 2]

    dws = (dw1_hbm, dw2_hbm)

    def reducer(j):
        st = {}

        def exchange(name, g, base, peers, n, src, dst):
            lst = st.setdefault(name, {}).setdefault(g, [])
            for k in range(1, n):
                lst.append(rcopy(src(k), dst(k), as_sem.at[j, g, base + k - 1],
                                 ar_sem.at[j, g, base + k - 1], peers(k)))
            start(lst)

        def core_send():
            c = rcopy(part.at[j, ds8(other * HALF, HALF)], crecv.at[j],
                      cs_sem.at[j, 0], cr_sem.at[j, 0], core_peer)
            st["core"] = c
            start([c])

        def p1():
            st["core"].wait_recv()
            for i in range(0, HALF, 216):
                hsum[j, pl.ds(i, 216)] = part[j, ds8(ci * HALF + i, 216)] + crecv[j, pl.ds(i, 216)]
            for g in range(2):
                peers, me, n = ring(g, 0)
                exchange("p1", g, 0, peers, n,
                         lambda k: hsum.at[j, ds8(g * GRP + ((me + k) % n) * 216, 216)],
                         lambda k: r1.at[j, g, k - 1])

        def p2():
            for g in range(2):
                recv(st["p1"][g])
                _, me, n = ring(g, 0)
                tot = hsum[j, ds8(g * GRP + me * 216, 216)]
                for k in range(n - 1):
                    tot = tot + r1[j, g, k]
                s1[j, g, pl.ds(0, 216)] = tot
                s1[j, g, pl.ds(216, 8)] = jnp.zeros((8, NC), F32)
                peers, me, n = ring(g, 1)
                exchange("p2", g, 3, peers, n,
                         lambda k: s1.at[j, g, ds8(((me + k) % n) * 56, 56)],
                         lambda k: r2.at[j, g, k - 1])

        def p3():
            for g in range(2):
                recv(st["p2"][g])
                _, me, n = ring(g, 1)
                tot = s1[j, g, ds8(me * 56, 56)]
                for k in range(n - 1):
                    tot = tot + r2[j, g, k]
                s2[j, g, pl.ds(0, 56)] = tot
                s2[j, g, pl.ds(56, 8)] = jnp.zeros((8, NC), F32)
                exchange("p3", g, 6, z_peer, nz,
                         lambda k: s2.at[j, g, ds8(((zi + k) % nz) * 8, 8)],
                         lambda k: r3.at[j, g, k - 1])

        def g3():
            for g in range(2):
                recv(st["p3"][g])
                tot = s2[j, g, ds8(zi * 8, 8)]
                for k in range(nz - 1):
                    tot = tot + r3[j, g, k]
                t2[j, g, ds8(zi * 8, 8)] = tot
                exchange("g3", g, 13, z_peer, nz,
                         lambda k: t2.at[j, g, ds8(zi * 8, 8)],
                         lambda k: t2.at[j, g, ds8(zi * 8, 8)])

        def g2():
            for g in range(2):
                recv(st["g3"][g])
                peers, me, n = ring(g, 1)
                t1[j, g, ds8(me * 56, 56)] = t2[j, g, pl.ds(0, 56)]
                exchange("g2", g, 20, peers, n,
                         lambda k: t2.at[j, g, pl.ds(0, 56)],
                         lambda k: t1.at[j, g, ds8(me * 56, 56)])

        def g1():
            for g in range(2):
                recv(st["g2"][g])
                peers, me, n = ring(g, 0)
                th[j, ds8(g * GRP + me * 216, 216)] = t1[j, g, pl.ds(0, 216)]
                exchange("g1", g, 23, peers, n,
                         lambda k: t1.at[j, g, pl.ds(0, 216)],
                         lambda k: th.at[j, ds8(g * GRP + me * 216, 216)])

        def core_gather():
            for g in range(2):
                recv(st["g1"][g])
            dst = dws[j].at[ds8(ci * HALF, HALF)]
            c = rcopy(th.at[j], dst, cs_sem.at[j, 1], cr_sem.at[j, 1], core_peer)
            st["last"] = c
            start([c])
            put_out(th.at[j], dst, j)

        def finish():
            st["last"].wait_recv()

        return [core_send, p1, p2, p3, g3, g2, g1, core_gather, finish]

    outs = []

    def put_out(src, dst, n):
        c = pltpu.make_async_copy(src, dst, out_sem.at[n])
        c.start()
        outs.append(c)

    red1, red2 = reducer(0), reducer(1)

    widen_local(xe, xc)
    recv(hx)
    widen_halo(xe, xc)
    conv(xc, w1f, fin_a)
    widen_local(ge, gc)
    start(hz)
    recv(hg)
    widen_halo(ge, gc)
    wgrad(zt, gc, 1, True)
    conv(gc, w2t, fin_da)
    red2[0]()
    wgrad(at, xc, 0, False)
    red2[1]()
    start(ha)
    widen_local(ze, zc)
    red1[0]()
    recv(hz)
    widen_halo(ze, zc)
    red2[2]()
    conv(zc, w2f, fin_add(xe, yv))
    red1[1]()
    red2[3]()
    put_out(yv, y_hbm, 2)
    widen_local(ae, ac)
    recv(ha)
    widen_halo(ae, ac)
    red2[4]()
    conv(ac, w1t, fin_add(ge, dxv))
    red1[2]()
    red2[5]()
    put_out(dxv, dx_hbm, 3)
    red1[3]()
    red2[6]()
    red1[4]()
    red2[7]()
    red1[5]()
    red1[6]()
    red1[7]()
    red2[8]()
    red1[8]()
    for c in outs:
        c.wait()
    for c in pending:
        c.wait_send()


def solution(mesh):
    nrow, ndep = mesh.shape['row'], mesh.shape['dep']
    ny = 4 if nrow >= 16 else 2
    nx, nz = ndep // 2, nrow // ny
    vol = P(None, 'dep', 'row', None, None)

    def local_step(x, w1, w2, g):
        ext = (NB, ND + 2, NR + 2, NW, NC)
        wide = (NB, ND + 2, NR + 2, NW, 3 * NC)
        tile = (NB, ND, NR, NW, NC)
        V = pltpu.VMEM
        DMA = pltpu.SemaphoreType.DMA
        flops = 6 * 2 * NB * ND * NR * NW * ROWS * NC
        out = pl.pallas_call(
            functools.partial(kernel, nx, ny, nz),
            out_shape=(jax.ShapeDtypeStruct(tile, BF16), jax.ShapeDtypeStruct(tile, BF16),
                       jax.ShapeDtypeStruct((ROWS, NC), F32), jax.ShapeDtypeStruct((ROWS, NC), F32)),
            in_specs=[pl.BlockSpec(memory_space=pl.ANY)] * 4,
            out_specs=(pl.BlockSpec(memory_space=pl.ANY),) * 4,
            scratch_shapes=[
                V(ext, BF16), V(ext, BF16), V(ext, BF16), V(ext, BF16),
                V(wide, BF16), V(wide, BF16), V(wide, BF16), V(wide, BF16),
                V((ROWS, NC), BF16), V((ROWS, NC), BF16),
                V((4608, 256), BF16), V((4608, 256), BF16), V((4608, 256), BF16), V((4608, 256), BF16),
                V((NB, ND, NR * NW, NC), F32),
                V((NC, 2048), BF16), V((NC, 2048), BF16),
                V((2, ROWS, NC), F32), V((2, HALF, NC), F32), V((2, HALF, NC), F32),
                V((2, 2, 3, 216, NC), F32), V((2, 2, 224, NC), F32),
                V((2, 2, 3, 56, NC), F32), V((2, 2, 64, NC), F32),
                V((2, 2, 7, 8, NC), F32), V((2, 2, 64, NC), F32),
                V((2, 2, 224, NC), F32), V((2, HALF, NC), F32),
                V(tile, BF16), V(tile, BF16),
                DMA((8,)), DMA((4, 8)), DMA((4, 8)), DMA((2, 2)), DMA((2, 2)),
                DMA((2, 2, 26)), DMA((2, 2, 26)), DMA((4,)),
            ],
            compiler_params=pltpu.CompilerParams(
                collective_id=0, has_side_effects=True, vmem_limit_bytes=67043328),
            cost_estimate=pl.CostEstimate(flops=flops, bytes_accessed=8 << 20, transcendentals=0),
            name="resblock",
        )(x, w1.reshape(ROWS, NC), w2.reshape(ROWS, NC), g)
        y, dx, dw1, dw2 = out
        return y, dx, dw1.reshape(w1.shape), dw2.reshape(w2.shape)

    return jax.shard_map(local_step, mesh=mesh, in_specs=(vol, P(), P(), vol),
                         out_specs=(vol, vol, P(), P()), check_vma=False)
```

```python
import functools

import jax
import jax.numpy as jnp
from jax import lax
from jax.experimental import pallas as pl
from jax.experimental.pallas import tpu as pltpu
from jax.sharding import PartitionSpec as P

MESH = pl.DeviceIdType.MESH
F32 = jnp.float32
BF16 = jnp.bfloat16

NB, ND, NR, NW, NC = 2, 2, 16, 32, 128
TAPS = 27
ROWS = TAPS * NC
PADDED = TAPS + 1
FIRST = (0, 10, 20)
COUNT = (10, 10, 8)
RINGS = (4, 4, 8)
ZP = 16
BASE = tuple(t * NC for t in FIRST)
OWN = tuple(t * NC for t in COUNT)
PIECE = tuple(n // r for n, r in zip(OWN, RINGS))
SUB = tuple(n // 4 for n in PIECE)
DIRS = (0, 1)
SLOTS = 4
PLANE = 9 * NC
TRIPLE = 3 * NC
CHUNKS = ((0, 0), (0, 8), (1, 0), (1, 8))
NEIGH = ((1, 0), (-1, 0), (0, 1), (0, -1), (1, 1), (1, -1), (-1, 1), (-1, -1))


def top(n):
    return pl.ds(0, n)


def inner(n):
    return pl.ds(1, n)


def others(n):
    return range(1, n)


def kernel(nx, ny, nz, x_hbm, w1_hbm, w2_hbm, g_hbm,
           y_out, dx_out, dw_out,
           xe, ge, ze, ae, xc, gc, zc, ac,
           w1r, w2r, w1f, w2f, w1t, w2t, v1f, v2f, v1t, v2t, gp, zt, at,
           acc1, acc2, part, crecv, hsum, r1, rz, r2, r15, r3, s1, s2, t2,
           in_sem, hs_sem, hr_sem, cs_sem, cr_sem, as_sem, ar_sem, greet_sem):
    row, dep = lax.axis_index("row"), lax.axis_index("dep")
    nrow, ndep = nz * ny, nx * 2
    zi, yi = row // ny, row % ny
    xi, ci = dep // 2, dep % 2

    def x_peer(k):
        return (row, ((xi + k) % nx) * 2 + ci)

    def y_peer(k):
        return (zi * ny + (yi + k) % ny, dep)

    def z_peer(k):
        return (((zi + k) % nz) * ny + yi, dep)

    core_peer = (row, xi * 2 + 1 - ci)

    def halo_peer(dr, dd):
        return ((row + dr + nrow) % nrow, (dep + dd + ndep) % ndep)

    cx = pltpu.make_async_copy(x_hbm, xe.at[:, inner(2), inner(NR)], in_sem.at[0])
    cg = pltpu.make_async_copy(g_hbm, ge.at[:, inner(2), inner(NR)], in_sem.at[1])
    cx.start()
    cg.start()

    def scope(name):
        return jax.named_scope(name)

    around = [peer(k) for peer, n in ((x_peer, nx), (y_peer, ny), (z_peer, nz)) for k in (1, n - 1)]
    partners = [halo_peer(a, b) for a, b in NEIGH] + around
    barrier = pltpu.get_barrier_semaphore()

    def signal(sem, peers):
        for p in peers:
            pl.semaphore_signal(sem, inc=1, device_id=p, device_id_type=MESH)

    signal(barrier, partners)
    cw = []

    def fetch(src, dst):
        c = pltpu.make_async_copy(src, dst, in_sem.at[2 + len(cw)])
        c.start()
        cw.append(c)

    lanes = (top(NC), pl.ds(NC, NC))

    def fetch_own(w, full):
        for d in DIRS:
            fetch(w.at[pl.ds((1 - d) * PLANE, 2 * PLANE)], full.at[:, lanes[d]])

    def fetch_edge(w, edge):
        for p in DIRS:
            for r in DIRS:
                fetch(w.at[pl.ds(2 * p * PLANE, PLANE)], edge.at[p, pl.ds(r * TRIPLE, PLANE), lanes[r]])

    fetch_own(w1_hbm, w1f)
    fetch(w2_hbm, w2r)
    with scope("barrier"):
        pl.semaphore_wait(barrier, len(partners))

    def greet(i):
        if i:
            pl.semaphore_wait(greet_sem.at[i - 1], len(around))
        if i < 3:
            signal(greet_sem.at[i], around)

    def halo_copies(slot, ext):
        out = []
        for k, (dr, dd) in enumerate(NEIGH):
            se, de = {1: (pl.ds(2, 1), top(1)), -1: (inner(1), pl.ds(3, 1)),
                      0: (inner(2), inner(2))}[dd]
            sr, tr = {1: (pl.ds(NR, 1), top(1)), -1: (inner(1), pl.ds(NR + 1, 1)),
                      0: (inner(NR), inner(NR))}[dr]
            out.append(pltpu.make_async_remote_copy(
                src_ref=ext.at[:, se, sr], dst_ref=ext.at[:, de, tr],
                send_sem=hs_sem.at[slot, min(k // 2, 1)], recv_sem=hr_sem.at[slot, min(k // 2, 1)],
                device_id=halo_peer(dr, dd), device_id_type=MESH))
        return out

    hx, hg, hz, ha = (halo_copies(i, e) for i, e in enumerate((xe, ge, ze, ae)))
    pending = []

    def start(copies):
        for c in copies:
            c.start()

    def drain(sem, region):
        pltpu.make_async_copy(region, region, sem).wait()

    def sent(sem, region):
        pending.append((sem, region))

    def start_halo(slot, ext, copies):
        start(copies)
        sent(hs_sem.at[slot, 0], ext.at[:, top(2), top(2)])
        sent(hs_sem.at[slot, 1], ext.at[:, top(2)])

    def recv_rows(slot, ext):
        drain(hr_sem.at[slot, 0], ext.at[:, top(2), top(2)])

    def recv_planes(slot, ext):
        drain(hr_sem.at[slot, 1], ext.at[:, top(2)])

    cx.wait()
    start_halo(0, xe, hx)
    cg.wait()
    start_halo(1, ge, hg)

    greet(0)
    fetch_edge(w1_hbm, v1f)
    soon = len(cw)
    fetch(w1_hbm, w1r)
    fetch_own(w2_hbm, w2f)
    fetch_edge(w2_hbm, v2f)

    blank = jnp.zeros((TRIPLE, NC), BF16)
    for edge in (v1f, v2f, v1t, v2t):
        for p in DIRS:
            for r in DIRS:
                edge[p, pl.ds((1 - r) * PLANE, TRIPLE), lanes[r]] = blank
    for j in range(2):
        part[j, pl.ds(ROWS, NC)] = jnp.zeros((NC, NC), F32)
    for c in cw[:3]:
        c.wait()

    def flip(raw, out, edge):
        for u in range(TAPS):
            block = raw[pl.ds((TAPS - 1 - u) * NC, NC), :].T
            plane, at_row = u // 9, (u % 9) * NC
            for d in DIRS:
                if plane >= 1 - d and plane <= 2 - d:
                    out[pl.ds((plane - 1 + d) * PLANE + at_row, NC), lanes[d]] = block
            if plane != 1:
                for r in DIRS:
                    edge[plane // 2, pl.ds(r * TRIPLE + at_row, NC), lanes[r]] = block

    flip(w2r, w2t, v2t)

    def widen(vals, store):
        v = vals.astype(F32)
        col = lax.broadcasted_iota(jnp.int32, v.shape, 1)
        left = jnp.where(col == 0, 0.0, pltpu.roll(v, 1, 1))
        right = jnp.where(col == NW - 1, 0.0, pltpu.roll(v, NW - 1, 1))
        store(0, left.astype(BF16))
        store(1, vals)
        store(2, right.astype(BF16))

    def widen_part(ext, out, b, e, r0, nr, keep):
        vals = ext[b, e, pl.ds(r0, nr)]
        if keep is not None:
            vals = jnp.where(keep, vals, jnp.zeros_like(vals))

        def store(j, piece):
            out[b, e, pl.ds(r0, nr), :, pl.ds(j * NC, NC)] = piece

        widen(vals, store)

    def widen_local(ext, out):
        for b in range(NB):
            for e in (1, 2):
                for r0 in (1, 9):
                    widen_part(ext, out, b, e, r0, 8, None)

    edges = ((0, row > 0), (NR + 1, row < nrow - 1))

    def widen_rows(ext, out):
        for b in range(NB):
            for e in (1, 2):
                for r0, keep in edges:
                    widen_part(ext, out, b, e, r0, 1, keep)

    def widen_planes(ext, out):
        for b in range(NB):
            for e, ek in ((0, dep > 0), (3, dep < ndep - 1)):
                for r0, keep in edges:
                    widen_part(ext, out, b, e, r0, 1, jnp.logical_and(ek, keep))
                for r0 in (1, 9):
                    widen_part(ext, out, b, e, r0, 8, ek)

    def conv_own(src, wts, acc):
        for i, (b, r0) in enumerate(CHUNKS):
            acc[i] = conv_part(src, wts, range(3), r0, b)

    def conv_part(src, wts, drs, r0, b):
        lhs = jnp.concatenate([src[b, e, pl.ds(r0 + dr, 8)].reshape(8 * NW, 3 * NC)
                               for e in (1, 2) for dr in drs], axis=1)
        rhs = jnp.concatenate([wts[pl.ds(e * PLANE + dr * TRIPLE, TRIPLE), :]
                               for e in DIRS for dr in drs], axis=0)
        return jnp.dot(lhs, rhs, preferred_element_type=F32)

    def conv_mid(src, wts, acc):
        for i, (b, r0) in enumerate(CHUNKS):
            acc[i] = conv_part(src, wts, (1,), r0, b)

    def conv_sides(src, wts, acc):
        for i, (b, r0) in enumerate(CHUNKS):
            acc[i] = acc[i] + conv_part(src, wts, (0, 2), r0, b)

    def conv_rest(src, edge, acc, finish):
        for b in range(NB):
            for d in range(ND):
                lhs = jnp.concatenate(
                    [jnp.concatenate([src[b, 3 * d, 2 * i + k] for i in range(NR // 2)], axis=0)
                     for k in range(4)], axis=1)
                pairs = jnp.dot(lhs, edge[d], preferred_element_type=F32)
                for h in range(2):
                    some = pairs[h * NC:(h + 1) * NC]
                    rows = jnp.concatenate([some[:, r * NC:(r + 1) * NC].reshape(4, 1, NW, NC)
                                            for r in DIRS], axis=1).reshape(8 * NW, NC)
                    finish(b, d, 8 * h, acc[2 * b + h, :, lanes[d]] + rows)

    def put(ref, b, d, r0, vals):
        ref[b, d, pl.ds(r0, 8)] = vals.reshape(8, NW, NC)

    def fin_a(b, d, r0, acc):
        a = acc.astype(BF16).astype(F32)
        c0, c1 = 0.7978845608028654, 0.044715
        sq = a * a
        th_ = jnp.tanh(c0 * (a + c1 * (sq * a)))
        cdf = 0.5 * (1.0 + th_)
        z = (a * cdf).astype(BF16)
        slope = cdf + (0.5 * a) * (1.0 - th_ * th_) * (c0 * (1.0 + (3.0 * c1) * sq))
        gp[b, d, pl.ds(r0 * NW, 8 * NW)] = slope
        put(ze, b, d + 1, r0 + 1, z)
        zt[:, pl.ds((d * NB + b) * 512 + r0 * NW, 8 * NW)] = z.T

    def fin_da(b, d, r0, acc):
        da = (acc * gp[b, d, pl.ds(r0 * NW, 8 * NW)]).astype(BF16)
        put(ae, b, d + 1, r0 + 1, da)
        at[:, pl.ds((d * NB + b) * 512 + r0 * NW, 8 * NW)] = da.T

    def fin_add(base, out):
        def fin(b, d, r0, acc):
            res = base[b, d + 1, pl.ds(r0 + 1, 8)].reshape(8 * NW, NC).astype(F32)
            out[pl.ds((b * ND + d) * 512 + r0 * NW, 8 * NW), :] = (acc + res).astype(BF16)
        return fin

    def tap_rhs(src, u):
        ud, dr, dw = u // 9, (u // 3) % 3, u % 3
        return jnp.concatenate(
            [src[b, d + ud, pl.ds(dr, NR), :, pl.ds(dw * NC, NC)].reshape(NR * NW, NC)
             for d in range(ND) for b in range(NB)], axis=0)

    def wgrad(lhs_t, src, j, g, flipped):
        lhs = lhs_t[...]
        taps = [t for t in range(FIRST[g], FIRST[g] + COUNT[g]) if t < TAPS]
        for n in range(0, len(taps), 2):
            pair = taps[n:n + 2]
            rhs = jnp.concatenate(
                [tap_rhs(src, TAPS - 1 - t if flipped else t) for t in pair], axis=1)
            out = jnp.dot(lhs, rhs, preferred_element_type=F32)
            for m, t in enumerate(pair):
                block = out[:, m * NC:(m + 1) * NC]
                part[j, pl.ds(t * NC, NC), :] = block if flipped else block.T

    def rcopy(src, dst, ssem, rsem, peer):
        return pltpu.make_async_remote_copy(src_ref=src, dst_ref=dst, send_sem=ssem,
                                            recv_sem=rsem, device_id=peer, device_id_type=MESH)

    def ds8(base, size):
        return pl.ds(pl.multiple_of(base, 8), size)

    rings = ((x_peer, xi), (y_peer, yi), (z_peer, zi))

    def reducer(n, j, g):
        own, piece, sub, n1 = OWN[g], PIECE[g], SUB[g], RINGS[g]
        half = piece // 2
        base = BASE[g]
        dw_mine = dw_out.at[j]
        (peer1, me1), (peer2, me2) = rings[g], rings[(1, 0, 0)[g]]
        sides = (peer1(1), peer1(n1 - 1))
        everything = crecv.at[n, top(own)]
        got2, got3, got15 = r2.at[n], r3.at[n], r15.at[n]

        def sems(phase, i):
            return as_sem.at[n, phase], ar_sem.at[n, i]

        def arrived(i, region):
            drain(ar_sem.at[n, i], region)

        def exchange(phase, i, peers, n, src, dst):
            start([rcopy(src(k), dst(k), *sems(phase, i), peers(k)) for k in others(n)])

        def core_send():
            start([rcopy(part.at[j, pl.ds(base, own)], everything,
                         cs_sem.at[n, 0], cr_sem.at[n, 0], core_peer)])

        def rows_of(k, h):
            return ds8(((me1 + k) % n1) * piece + h * half, half)

        def rows_at(k):
            return ds8(((me1 + k) % n1) * piece, piece)

        def from_core():
            drain(cr_sem.at[n, 0], everything)
            for i in range(0, own, piece):
                hsum[n, pl.ds(i, piece)] = part[j, pl.ds(base + i, piece)] + crecv[n, pl.ds(i, piece)]

        def absorb(rows, more):
            hsum[n, rows] = hsum[n, rows] + more

        def ring_copy(i):
            k, h = ((2, 0), (2, 1), (1, 1), (3, 0), (1, 0), (3, 1))[i]
            return rcopy(hsum.at[n, rows_of(k, h)], r1.at[n, i],
                         *sems(0, min(i, 2)), sides[i % 2])

        def p1():
            from_core()
            start([ring_copy(i) for i in range(4)])

        def p1m():
            for i, k in enumerate((1, 3)):
                arrived(i, r1.at[n, i])
                absorb(rows_of(k, i), r1[n, i])
                start([ring_copy(4 + i)])

        def flow(d, s):
            return (4 - s) if d == 0 else (4 + s)

        def z_copy(d, s, src, part_rows):
            start([rcopy(hsum.at[n, src], rz.at[n, d, s, part_rows], *sems(0, 4 * d + s), sides[d])])

        def part_of(h):
            return pl.ds(h * half, half)

        def z0():
            from_core()
            for d in DIRS:
                z_copy(d, 0, rows_of(4, d), part_of(d))
            for d in DIRS:
                z_copy(d, 1, rows_of(flow(d, 1), 1 - d), part_of(1 - d))

        def z1():
            for d in DIRS:
                arrived(4 * d, rz.at[n, d, 0, part_of(d)])
                rows = rows_of(flow(d, 1), d)
                absorb(rows, rz[n, d, 0, part_of(d)])
                z_copy(d, 1, rows, part_of(d))

        def z_step(s):
            def step():
                for d in DIRS:
                    arrived(4 * d + s - 1, rz.at[n, d, s - 1])
                    rows = rows_at(flow(d, s))
                    absorb(rows, rz[n, d, s - 1])
                    z_copy(d, s, rows, top(piece))
            return step

        def plane(phase, i, src, dst):
            for kx in range(4):
                for ky in range(4):
                    k = 4 * kx + ky
                    if k:
                        px, py = (xi + kx) % nx, (yi + ky) % nx
                        start([rcopy(src(px * 4 + py), dst(k - 1), *sems(phase, i),
                                     (zi * ny + py, px * 2 + ci))])

        def z_end():
            for d in DIRS:
                arrived(4 * d + 3, rz.at[n, d, 3])
            s1[n, top(piece)] = hsum[n, rows_at(0)] + rz[n, 0, 3] + rz[n, 1, 3]
            plane(1, 8, lambda q: s1.at[n, ds8(q * 8, 8)], lambda k: r15.at[n, k])

        def z_spread():
            arrived(8, got15)
            q = (xi * 4 + yi) * 8
            tot = s1[n, ds8(q, 8)]
            for k in range(15):
                tot = tot + r15[n, k]
            t2[n, top(8)] = tot
            rows = ds8(base + me1 * piece + q, 8)
            plane(2, 9, lambda q: t2.at[n, top(8)], lambda k: dw_mine.at[rows])
            dw_out[j, rows] = tot

        def p2():
            arrived(2, r1.at[n, pl.ds(2, 4)])
            for h, (u, v) in enumerate(((3, 4), (2, 5))):
                s1[n, part_of(h)] = hsum[n, rows_of(0, h)] + r1[n, u] + r1[n, v]
            exchange(1, 8, peer2, 4, lambda k: s1.at[n, ds8(((me2 + k) % nx) * sub, sub)],
                     lambda k: r2.at[n, k - 1])

        def p3():
            arrived(8, got2)
            tot = s1[n, ds8(me2 * sub, sub)]
            for k in range(3):
                tot = tot + r2[n, k]
            s2[n, top(sub)] = tot
            s2[n, pl.ds(sub, nz * ZP - sub)] = jnp.zeros((nz * ZP - sub, NC), F32)
            exchange(2, 9, z_peer, nz, lambda k: s2.at[n, ds8(((zi + k) % nz) * ZP, ZP)],
                     lambda k: r3.at[n, k - 1])

        def g3():
            arrived(9, got3)
            mine = ds8(zi * ZP, ZP)
            tot = s2[n, mine]
            for k in range(nz - 1):
                tot = tot + r3[n, k]
            t2[n, mine] = tot
            exchange(3, 10, z_peer, nz, lambda k: t2.at[n, mine], lambda k: t2.at[n, mine])

        def out_rows(k, h=0, size=piece):
            return ds8(base + ((me1 + k) % n1) * piece + h * half, size)

        def pass_on(rows, i, d):
            start([rcopy(dw_mine.at[rows], dw_mine.at[rows], *sems(3 if g == 2 else 5, i), sides[d])])

        def to_core(rows):
            start([rcopy(dw_mine.at[rows], dw_mine.at[rows], cs_sem.at[n, 1], cr_sem.at[n, 1], core_peer)])

        def g2():
            arrived(10, got3)
            rows = ds8(base + me1 * piece + me2 * sub, sub)
            exchange(4, 11, peer2, 4, lambda k: t2.at[n, top(sub)], lambda k: dw_mine.at[rows])
            dw_out[j, rows] = t2[n, top(sub)]

        def g1():
            arrived(11, got2)
            for i in range(4):
                pass_on(out_rows(0, (i + i // 2) % 2, half), 12 + min(i, 2), i % 2)
            to_core(out_rows(0))

        def g1m():
            for d, k in enumerate((3, 1)):
                rows = out_rows(k, d, half)
                arrived(12 + d, dw_mine.at[rows])
                pass_on(rows, 14, d)
                to_core(rows)

        def gather_end():
            arrived(14, r1.at[n, pl.ds(2, 4)])
            for k, h in ((3, 1), (1, 0)):
                to_core(out_rows(k, h, half))
            to_core(out_rows(2))

        def w0():
            arrived(9, got15)
            for d in DIRS:
                pass_on(out_rows(0), 12 + 4 * d, d)
            to_core(out_rows(0))

        def w_step(s):
            def step():
                for d in DIRS:
                    k = 8 - s if d == 0 else s
                    whole = out_rows(k)
                    arrived(12 + 4 * d + s - 1, dw_mine.at[whole])
                    pass_on(whole if s < 3 else out_rows(k, d, half), 12 + 4 * d + s, d)
                    to_core(whole)
            return step

        def w_end():
            for d in DIRS:
                arrived(15 + 4 * d, dw_mine.at[out_rows(4, d, half)])
            to_core(out_rows(4))

        def sent_all():
            ring_bytes = crecv.at[n, top((n1 - 1) * piece)]
            middle = (got15, got15) if g == 2 else (got2, got3, got3, got2)
            for i, region in enumerate((ring_bytes,) + middle + (ring_bytes,)):
                drain(as_sem.at[n, i], region)
            drain(cs_sem.at[n, 1], everything)

        def finish():
            drain(cr_sem.at[n, 1], everything)
            drain(cs_sem.at[n, 0], everything)

        steps = dict(cs=core_send, fin=finish, end=sent_all)
        if g == 2:
            steps.update(p1=z0, z1=z1, z2=z_step(2), z3=z_step(3), p2=z_end, p3=z_spread, g1=w0, w1=w_step(1),
                         w2=w_step(2), w3=w_step(3), gc=w_end)
        else:
            steps.update(p1=p1, p1m=p1m, p2=p2, p3=p3, g3=g3, g2=g2, g1=g1, g1m=g1m, gc=gather_end)
        return steps

    table = {}
    for i, c in enumerate("ABYabz"):
        g = i % 3
        table[c] = (g + (c == "Y"), int(c.isupper()), g, int(c not in "AB"))
    chains = {name: reducer(*spec[:3]) for name, spec in table.items()}

    def sums(*words):
        for word in words:
            names, step = word.split(".")
            for c in names:
                with scope(c + "_" + step):
                    chains[c][step]()

    def on_core(core, *words):
        @pl.when(ci == core)
        def _():
            sums(*words)

    def give(c):
        on_core(1 - table[c][3], c + ".cs")

    with scope("xlocal"):
        widen_local(xe, xc)
        conv_mid(xc, w1f, acc1)
    with scope("glocal"):
        widen_local(ge, gc)
        conv_mid(gc, w2t, acc2)
    greet(1)
    with scope("xrows"):
        recv_rows(0, xe)
    with scope("c1own"):
        widen_rows(xe, xc)
        conv_sides(xc, w1f, acc1)
    with scope("grows"):
        recv_rows(1, ge)
    with scope("ct2own"):
        widen_rows(ge, gc)
        conv_sides(gc, w2t, acc2)
    greet(2)
    for c in cw[3:soon]:
        c.wait()
    with scope("xplanes"):
        recv_planes(0, xe)
    with scope("c1rest"):
        widen_planes(xe, xc)
        conv_rest(xc, v1f, acc1, fin_a)
    greet(3)
    with scope("gplanes"):
        recv_planes(1, ge)
    with scope("gplanesw"):
        widen_planes(ge, gc)
    start_halo(2, ze, hz)
    for c in "YBA":
        with scope("d2"):
            wgrad(zt, gc, 1, table[c][2], True)
        give(c)
    with scope("ct2rest"):
        conv_rest(gc, v2t, acc2, fin_da)
    start_halo(3, ae, ha)
    on_core(0, "B.p1")
    on_core(1, "Y.p1")
    with scope("d1z"):
        wgrad(at, xc, 0, 2, False)
    give("z")
    on_core(0, "A.p1")
    with scope("d1b"):
        wgrad(at, xc, 0, 1, False)
    give("b")
    with scope("d1a"):
        wgrad(at, xc, 0, 0, False)
    give("a")
    on_core(1, "Y.z1")
    with scope("late"):
        for c in cw[soon:]:
            c.wait()
        flip(w1r, w1t, v1t)
    with scope("zhalo"):
        widen_local(ze, zc)
        recv_rows(2, ze)
        widen_rows(ze, zc)
    on_core(1, "z.p1")
    with scope("c2own"):
        conv_own(zc, w2f, acc1)
    on_core(0, "B.p1m", "A.p1m")
    on_core(1, "b.p1")
    with scope("zplanes"):
        recv_planes(2, ze)
        widen_planes(ze, zc)
    on_core(1, "a.p1", "Y.z2")
    with scope("c2rest"):
        conv_rest(zc, v2f, acc1, fin_add(xe, y_out))
    on_core(1, "z.z1")
    with scope("ahalo"):
        widen_local(ae, ac)
        recv_rows(3, ae)
        widen_rows(ae, ac)
    with scope("ct1own"):
        conv_own(ac, w1t, acc2)
    on_core(0, "BA.p2")
    on_core(1, "Y.z3", "ba.p1m")
    with scope("aplanes"):
        recv_planes(3, ae)
        widen_planes(ae, ac)
    on_core(1, "z.z2")
    with scope("ct1rest"):
        conv_rest(ac, v1t, acc2, fin_add(ge, dx_out))
    on_core(0, "BA.p3", "BA.g3", "BA.g2", "BA.g1", "BA.g1m", "BA.gc")
    on_core(1, "Y.p2", "z.z3", "ba.p2", "Y.p3", "z.p2", "ba.p3", "Y.g1", "z.p3", "ba.g3",
            "Y.w1", "z.g1", "ba.g2", "Y.w2", "z.w1", "ba.g1", "Y.w3", "z.w2", "Y.gc", "ba.g1m",
            "z.w3", "z.gc", "ba.gc")
    on_core(0, "Yzba.fin", "AB.end")
    on_core(1, "AB.fin", "Yzba.end")
    with scope("tail"):
        for sem, region in pending:
            drain(sem, region)


def settle(y, dx, dw, *refs):
    rows = top(ROWS)
    copies = [pltpu.make_async_copy(src, dst, refs[4].at[n])
              for n, (src, dst) in enumerate(zip((y, dx, dw.at[0, rows], dw.at[1, rows]), refs[:4]))]
    for c in copies:
        c.start()
    for c in copies:
        c.wait()


def solution(mesh):
    nrow, ndep = mesh.shape['row'], mesh.shape['dep']
    ny = 4 if nrow >= 16 else 2
    nx, nz = ndep // 2, nrow // ny
    vol = P(None, 'dep', 'row', None, None)

    def local_step(x, w1, w2, g):
        ext = (NB, ND + 2, NR + 2, NW, NC)
        wide = (NB, ND + 2, NR + 2, NW, 3 * NC)
        tile = (NB, ND, NR, NW, NC)
        V = pltpu.VMEM
        DMA = pltpu.SemaphoreType.DMA
        flops = 6 * 2 * NB * ND * NR * NW * ROWS * NC
        out = pl.pallas_call(
            functools.partial(kernel, nx, ny, nz),
            out_shape=(V((2048, NC), BF16),) * 2 + (V((2, PADDED * NC, NC), F32),),
            in_specs=[pl.BlockSpec(memory_space=pl.ANY)] * 4,
            out_specs=(pl.BlockSpec(memory_space=V),) * 3,
            scratch_shapes=[V(ext, BF16)] * 4 + [V(wide, BF16)] * 4 + [V((ROWS, NC), BF16)] * 2
            + [V((2 * PLANE, 2 * NC), BF16)] * 4 + [V((2, 4 * TRIPLE, 2 * NC), BF16)] * 4
            + [V((NB, ND, NR * NW, NC), F32)] + [V((NC, 2048), BF16)] * 2
            + [V((4, 256, 256), F32)] * 2
            + [V((2, PADDED * NC, NC), F32)] + [V((SLOTS, OWN[0], NC), F32)] * 2 + [
                V((SLOTS, 6, PIECE[0] // 2, NC), F32), V((SLOTS, 2, 4, PIECE[2], NC), F32),
                V((SLOTS, 3, SUB[0], NC), F32),
                V((SLOTS, 15, 8, NC), F32), V((SLOTS, nz - 1, ZP, NC), F32),
                V((SLOTS, PIECE[0], NC), F32), V((SLOTS, nz * ZP, NC), F32), V((SLOTS, nz * ZP, NC), F32),
                DMA((16,)), DMA((4, 2)), DMA((4, 2)), DMA((SLOTS, 2)), DMA((SLOTS, 2)),
                DMA((SLOTS, 6)), DMA((SLOTS, 20)), pltpu.SemaphoreType.REGULAR((3,))],
            compiler_params=pltpu.CompilerParams(
                collective_id=0, has_side_effects=True, vmem_limit_bytes=58720256),
            cost_estimate=pl.CostEstimate(flops=flops, bytes_accessed=8000000, transcendentals=0),
            name="resblock",
        )(x, w1.reshape(ROWS, NC), w2.reshape(ROWS, NC), g)
        shapes = [jax.ShapeDtypeStruct((n, NC), t) for n, t in ((2048, BF16), (ROWS, F32)) for _ in "ab"]
        y, dx, dw1, dw2 = pl.pallas_call(
            settle,
            out_shape=shapes,
            in_specs=[pl.BlockSpec(memory_space=V)] * 3,
            out_specs=[pl.BlockSpec(memory_space=pl.ANY)] * 4,
            scratch_shapes=[DMA((4,))],
            compiler_params=pltpu.CompilerParams(vmem_limit_bytes=1048576),
            cost_estimate=pl.CostEstimate(flops=0, bytes_accessed=8000000, transcendentals=0),
            name="settle",
        )(*out)
        return y.reshape(tile), dx.reshape(tile), dw1.reshape(w1.shape), dw2.reshape(w2.shape)

    return jax.shard_map(local_step, mesh=mesh, in_specs=(vol, P(), P(), vol),
                         out_specs=(vol, vol, P(), P()), check_vma=False)
```

```python
import functools

import jax
import jax.numpy as jnp
from jax import lax
from jax.experimental import pallas as pl
from jax.experimental.pallas import tpu as pltpu
from jax.sharding import PartitionSpec as P

MESH = pl.DeviceIdType.MESH
F32 = jnp.float32
BF16 = jnp.bfloat16

NB, ND, NR, NW, NC = 2, 2, 16, 32, 128
TAPS = 27
ROWS = TAPS * NC
FIRST = (0, 9, 19)
COUNT = (9, 10, 8)
RINGS = (4, 4, 8)
ZP = 16
BASE = tuple(t * NC for t in FIRST)
OWN = tuple(t * NC for t in COUNT)
PIECE = tuple(n // r for n, r in zip(OWN, RINGS))
SUB = tuple(n // 4 for n in PIECE)
DIRS = (0, 1)
SLOTS = 4
PLANE = 9 * NC
TRIPLE = 3 * NC
CHUNKS = ((0, 0), (0, 8), (1, 0), (1, 8))
NEIGH = ((1, 0), (-1, 0), (1, 1), (1, -1), (-1, 1), (-1, -1), (0, 1), (0, -1))


def top(n):
    return pl.ds(0, n)


def inner(n):
    return pl.ds(1, n)


def others(n):
    return range(1, n)


def kernel(nx, ny, nz, x_hbm, w1_hbm, w2_hbm, g_hbm,
           y_out, dx_out, dw_out,
           xe, ge, ze, ae, xc, gc, zc, ac,
           w1r, w2r, w1f, w2f, w1t, w2t, v1f, v2f, v1t, v2t, gp, zt, at,
           acc1, acc2, part, crecv, hsum, r1, rz, r2, r15, r3, s1, s2, t2,
           in_sem, hs_sem, hr_sem, cs_sem, cr_sem, as_sem, ar_sem, az_sem, greet_sem):
    row, dep = lax.axis_index("row"), lax.axis_index("dep")
    nrow, ndep = nz * ny, nx * 2
    zi, yi = row // ny, row % ny
    xi, ci = dep // 2, dep % 2

    def x_peer(k):
        return (row, ((xi + k) % nx) * 2 + ci)

    def y_peer(k):
        return (zi * ny + (yi + k) % ny, dep)

    def z_peer(k):
        return (((zi + k) % nz) * ny + yi, dep)

    core_peer = (row, xi * 2 + 1 - ci)

    def halo_peer(dr, dd):
        return ((row + dr + nrow) % nrow, (dep + dd + ndep) % ndep)

    cx = pltpu.make_async_copy(x_hbm, xe.at[:, inner(2), inner(NR)], in_sem.at[0])
    cg = pltpu.make_async_copy(g_hbm, ge.at[:, inner(2), inner(NR)], in_sem.at[1])
    cx.start()
    cg.start()

    def scope(name):
        return jax.named_scope(name)

    around = [peer(k) for peer, n in ((x_peer, nx), (y_peer, ny), (z_peer, nz)) for k in (1, n - 1)]
    partners = [halo_peer(a, b) for a, b in NEIGH] + around
    barrier = pltpu.get_barrier_semaphore()

    def signal(sem, peers):
        for p in peers:
            pl.semaphore_signal(sem, inc=1, device_id=p, device_id_type=MESH)

    signal(barrier, partners)
    cw = []

    def fetch(src, dst):
        c = pltpu.make_async_copy(src, dst, in_sem.at[2 + len(cw) % 7])
        c.start()
        cw.append(c)

    lanes = (top(NC), pl.ds(NC, NC))

    def fetch_own(w, full):
        for d in DIRS:
            fetch(w.at[pl.ds((1 - d) * PLANE, 2 * PLANE)], full.at[:, lanes[d]])

    def fetch_edge(w, edge):
        for p in DIRS:
            for r in DIRS:
                fetch(w.at[pl.ds(2 * p * PLANE, PLANE)], edge.at[p, pl.ds(r * TRIPLE, PLANE), lanes[r]])

    fetch_own(w1_hbm, w1f)
    fetch(w2_hbm, w2r)
    with scope("barrier"):
        pl.semaphore_wait(barrier, len(partners))

    def greet(i):
        if i:
            pl.semaphore_wait(greet_sem.at[i - 1], len(around))
        if i < 3:
            signal(greet_sem.at[i], around)

    def halo_copies(slot, ext):
        out = []
        for k, (dr, dd) in enumerate(NEIGH):
            se, de = {1: (pl.ds(2, 1), top(1)), -1: (inner(1), pl.ds(3, 1)),
                      0: (inner(2), inner(2))}[dd]
            sr, tr = {1: (pl.ds(NR, 1), top(1)), -1: (inner(1), pl.ds(NR + 1, 1)),
                      0: (inner(NR), inner(NR))}[dr]
            out.append(pltpu.make_async_remote_copy(
                src_ref=ext.at[:, se, sr], dst_ref=ext.at[:, de, tr],
                send_sem=hs_sem.at[slot], recv_sem=hr_sem.at[slot, min(k // 2, 1)],
                device_id=halo_peer(dr, dd), device_id_type=MESH))
        return out

    hx, hg, hz, ha = (halo_copies(i, e) for i, e in enumerate((xe, ge, ze, ae)))
    pending = []

    def start(copies):
        for c in copies:
            c.start()

    def drain(sem, region):
        pltpu.make_async_copy(region, region, sem).wait()

    def sent(sem, region):
        pending.append((sem, region))

    def start_halo(slot, ext, copies):
        start(copies)
        sent(hs_sem.at[slot], ext.at[:, :, top((2 * NR + 8) // 4)])

    def recv_rows(slot, ext):
        drain(hr_sem.at[slot, 0], ext.at[:, top(2), top(2)])

    def recv_planes(slot, ext):
        drain(hr_sem.at[slot, 1], ext.at[:, top(2)])

    cx.wait()
    start_halo(0, xe, hx)
    cg.wait()
    start_halo(1, ge, hg)

    greet(0)
    fetch_edge(w1_hbm, v1f)
    soon = len(cw)

    blank = jnp.zeros((TRIPLE, NC), BF16)
    for edge in (v1f, v2f, v1t, v2t):
        for p in DIRS:
            for r in DIRS:
                edge[p, pl.ds((1 - r) * PLANE, TRIPLE), lanes[r]] = blank
    for c in cw[:3]:
        c.wait()

    def flip(raw, out, edge):
        for u in range(TAPS):
            block = raw[pl.ds((TAPS - 1 - u) * NC, NC), :].T
            plane, at_row = u // 9, (u % 9) * NC
            for d in DIRS:
                if plane >= 1 - d and plane <= 2 - d:
                    out[pl.ds((plane - 1 + d) * PLANE + at_row, NC), lanes[d]] = block
            if plane != 1:
                for r in DIRS:
                    edge[plane // 2, pl.ds(r * TRIPLE + at_row, NC), lanes[r]] = block

    flip(w2r, w2t, v2t)

    def widen(vals, store):
        v = vals.astype(F32)
        col = lax.broadcasted_iota(jnp.int32, v.shape, 1)
        left = jnp.where(col == 0, 0.0, pltpu.roll(v, 1, 1))
        right = jnp.where(col == NW - 1, 0.0, pltpu.roll(v, NW - 1, 1))
        store(0, left.astype(BF16))
        store(1, vals)
        store(2, right.astype(BF16))

    def widen_part(ext, out, b, e, r0, nr, keep):
        vals = ext[b, e, pl.ds(r0, nr)]
        if keep is not None:
            vals = jnp.where(keep, vals, jnp.zeros_like(vals))

        def store(j, piece):
            out[b, e, pl.ds(r0, nr), :, pl.ds(j * NC, NC)] = piece

        widen(vals, store)

    def widen_local(ext, out):
        for b in range(NB):
            for e in (1, 2):
                for r0 in (1, 9):
                    widen_part(ext, out, b, e, r0, 8, None)

    edges = ((0, row > 0), (NR + 1, row < nrow - 1))

    def widen_rows(ext, out):
        for b in range(NB):
            for e in (1, 2):
                for r0, keep in edges:
                    widen_part(ext, out, b, e, r0, 1, keep)

    def widen_planes(ext, out):
        for b in range(NB):
            for e, ek in ((0, dep > 0), (3, dep < ndep - 1)):
                for r0, keep in edges:
                    widen_part(ext, out, b, e, r0, 1, jnp.logical_and(ek, keep))
                for r0 in (1, 9):
                    widen_part(ext, out, b, e, r0, 8, ek)

    def conv_own(src, wts, acc):
        for i, (b, r0) in enumerate(CHUNKS):
            acc[i] = conv_part(src, wts, range(3), r0, b)

    def conv_part(src, wts, drs, r0, b):
        lhs = jnp.concatenate([src[b, e, pl.ds(r0 + dr, 8)].reshape(8 * NW, 3 * NC)
                               for e in (1, 2) for dr in drs], axis=1)
        rhs = jnp.concatenate([wts[pl.ds(e * PLANE + dr * TRIPLE, TRIPLE), :]
                               for e in DIRS for dr in drs], axis=0)
        return jnp.dot(lhs, rhs, preferred_element_type=F32)

    def conv_mid(src, wts, acc):
        for i, (b, r0) in enumerate(CHUNKS):
            acc[i] = conv_part(src, wts, (1,), r0, b)

    def conv_sides(src, wts, acc):
        for i, (b, r0) in enumerate(CHUNKS):
            acc[i] = acc[i] + conv_part(src, wts, (0, 2), r0, b)

    def conv_rest(src, edge, acc, finish):
        for b in range(NB):
            for d in range(ND):
                lhs = jnp.concatenate(
                    [jnp.concatenate([src[b, 3 * d, 2 * i + k] for i in range(NR // 2)], axis=0)
                     for k in range(4)], axis=1)
                pairs = jnp.dot(lhs, edge[d], preferred_element_type=F32)
                for h in range(2):
                    some = pairs[h * NC:(h + 1) * NC]
                    rows = jnp.concatenate([some[:, r * NC:(r + 1) * NC].reshape(4, 1, NW, NC)
                                            for r in DIRS], axis=1).reshape(8 * NW, NC)
                    finish(b, d, 8 * h, acc[2 * b + h, :, lanes[d]] + rows)

    def put(ref, b, d, r0, vals):
        ref[b, d, pl.ds(r0, 8)] = vals.reshape(8, NW, NC)

    def fin_a(b, d, r0, acc):
        a = acc.astype(BF16).astype(F32)
        c0, c1 = 0.7978845608028654, 0.044715
        sq = a * a
        th_ = jnp.tanh(c0 * (a + c1 * (sq * a)))
        cdf = 0.5 * (1.0 + th_)
        z = (a * cdf).astype(BF16)
        slope = cdf + (0.5 * a) * (1.0 - th_ * th_) * (c0 * (1.0 + (3.0 * c1) * sq))
        gp[b, d, pl.ds(r0 * NW, 8 * NW)] = slope
        put(ze, b, d + 1, r0 + 1, z)
        zt[:, pl.ds((d * NB + b) * 512 + r0 * NW, 8 * NW)] = z.T

    def fin_da(b, d, r0, acc):
        da = (acc * gp[b, d, pl.ds(r0 * NW, 8 * NW)]).astype(BF16)
        put(ae, b, d + 1, r0 + 1, da)
        at[:, pl.ds((d * NB + b) * 512 + r0 * NW, 8 * NW)] = da.T

    def fin_add(base, out):
        def fin(b, d, r0, acc):
            res = base[b, d + 1, pl.ds(r0 + 1, 8)].reshape(8 * NW, NC).astype(F32)
            out[pl.ds((b * ND + d) * 512 + r0 * NW, 8 * NW), :] = (acc + res).astype(BF16)
        return fin

    def tap_rhs(src, u):
        ud, dr, dw = u // 9, (u // 3) % 3, u % 3
        return jnp.concatenate(
            [src[b, d + ud, pl.ds(dr, NR), :, pl.ds(dw * NC, NC)].reshape(NR * NW, NC)
             for d in range(ND) for b in range(NB)], axis=0)

    def wgrad(lhs_t, src, j, g, flipped):
        lhs = lhs_t[...]
        taps = [t for t in range(FIRST[g], FIRST[g] + COUNT[g]) if t < TAPS]
        for n in range(0, len(taps), 2):
            pair = taps[n:n + 2]
            rhs = jnp.concatenate(
                [tap_rhs(src, TAPS - 1 - t if flipped else t) for t in pair], axis=1)
            out = jnp.dot(lhs, rhs, preferred_element_type=F32)
            for m, t in enumerate(pair):
                block = out[:, m * NC:(m + 1) * NC]
                part[j, pl.ds(t * NC, NC), :] = block if flipped else block.T

    def rcopy(src, dst, ssem, rsem, peer):
        return pltpu.make_async_remote_copy(src_ref=src, dst_ref=dst, send_sem=ssem,
                                            recv_sem=rsem, device_id=peer, device_id_type=MESH)

    def ds8(base, size):
        return pl.ds(pl.multiple_of(base, 8), size)

    rings = ((x_peer, xi), (y_peer, yi), (z_peer, zi))

    def arrival(n, i):
        return (ar_sem if n < 2 else az_sem).at[n % 2, i]

    def reducer(n, j, g):
        own, piece, sub, n1 = OWN[g], PIECE[g], SUB[g], RINGS[g]
        half = piece // 2
        base = BASE[g]
        dw_mine = dw_out.at[j]
        (peer1, me1), (peer2, me2) = rings[g], rings[(1, 0, 0)[g]]
        sides = (peer1(1), peer1(n1 - 1))
        everything = crecv.at[n, top(own)]
        got2, got3, got15 = r2.at[n, :, top(sub)], r3.at[n], r15.at[n]

        def sems(phase, i):
            return as_sem.at[n], arrival(n, i)

        def arrived(i, region):
            drain(arrival(n, i), region)

        def exchange(phase, i, peers, n, src, dst):
            far_first = sorted(others(n), key=lambda k: -min(k, n - k))
            start([rcopy(src(k), dst(k), *sems(phase, i), peers(k)) for k in far_first])

        def core_send():
            start([rcopy(part.at[j, pl.ds(base, own)], everything,
                         cs_sem.at[n], cr_sem.at[n, 0], core_peer)])

        def rows_of(k, h):
            return ds8(((me1 + k) % n1) * piece + h * half, half)

        def rows_at(k):
            return ds8(((me1 + k) % n1) * piece, piece)

        def from_core():
            drain(cr_sem.at[n, 0], everything)
            for i in range(0, own, piece):
                hsum[n, pl.ds(i, piece)] = part[j, pl.ds(base + i, piece)] + crecv[n, pl.ds(i, piece)]

        def absorb(rows, more):
            hsum[n, rows] = hsum[n, rows] + more

        def ring_copy(i):
            k, h = ((2, 0), (2, 1), (1, 1), (3, 0), (1, 0), (3, 1))[i]
            return rcopy(hsum.at[n, rows_of(k, h)], r1.at[n, i, top(half)],
                         *sems(0, min(i, 2)), sides[i % 2])

        def p1():
            from_core()
            start([ring_copy(i) for i in range(4)])

        def p1m():
            for i, k in enumerate((1, 3)):
                arrived(i, r1.at[n, i, top(half)])
                absorb(rows_of(k, i), r1[n, i, top(half)])
                start([ring_copy(4 + i)])

        def flow(d, s):
            return (4 - s) if d == 0 else (4 + s)

        def z_copy(d, s, src, part_rows):
            start([rcopy(hsum.at[n, src], rz.at[n, d, s, part_rows], *sems(0, 4 * d + s), sides[d])])

        def part_of(h):
            return pl.ds(h * half, half)

        def z0():
            from_core()
            for d in DIRS:
                z_copy(d, 0, rows_of(4, d), part_of(d))
            for d in DIRS:
                z_copy(d, 1, rows_of(flow(d, 1), 1 - d), part_of(1 - d))

        def z1():
            for d in DIRS:
                arrived(4 * d, rz.at[n, d, 0, part_of(d)])
                rows = rows_of(flow(d, 1), d)
                absorb(rows, rz[n, d, 0, part_of(d)])
                z_copy(d, 1, rows, part_of(d))

        def z_step(s):
            def step():
                for d in DIRS:
                    arrived(4 * d + s - 1, rz.at[n, d, s - 1])
                    rows = rows_at(flow(d, s))
                    absorb(rows, rz[n, d, s - 1])
                    z_copy(d, s, rows, top(piece))
            return step

        def plane(phase, i, src, dst):
            for k in sorted(others(16), key=lambda k: -sum(min(q, nx - q) for q in divmod(k, nx))):
                px, py = (xi + k // nx) % nx, (yi + k % nx) % nx
                start([rcopy(src(px * 4 + py), dst(k - 1), *sems(phase, i), (zi * ny + py, px * 2 + ci))])

        def z_end():
            for d in DIRS:
                arrived(4 * d + 3, rz.at[n, d, 3])
            s1[n, top(piece)] = hsum[n, rows_at(0)] + rz[n, 0, 3] + rz[n, 1, 3]
            plane(1, 8, lambda q: s1.at[n, ds8(q * 8, 8)], lambda k: r15.at[n, k])

        def z_spread():
            arrived(8, got15)
            q = (xi * 4 + yi) * 8
            tot = s1[n, ds8(q, 8)]
            for k in range(15):
                tot = tot + r15[n, k]
            t2[n, top(8)] = tot
            rows = ds8(base + me1 * piece + q, 8)
            plane(2, 9, lambda q: t2.at[n, top(8)], lambda k: dw_mine.at[rows])
            dw_out[j, rows] = tot

        def p2():
            arrived(2, r1.at[n, pl.ds(2, 4), top(half)])
            for h, (u, v) in enumerate(((3, 4), (2, 5))):
                s1[n, part_of(h)] = hsum[n, rows_of(0, h)] + r1[n, u, top(half)] + r1[n, v, top(half)]
            exchange(1, 8, peer2, 4, lambda k: s1.at[n, ds8(((me2 + k) % nx) * sub, sub)],
                     lambda k: r2.at[n, k - 1, top(sub)])

        def p3():
            arrived(8, got2)
            tot = s1[n, ds8(me2 * sub, sub)]
            for k in range(3):
                tot = tot + r2[n, k, top(sub)]
            s2[n, top(sub)] = tot
            s2[n, pl.ds(sub, nz * ZP - sub)] = jnp.zeros((nz * ZP - sub, NC), F32)
            exchange(2, 9, z_peer, nz, lambda k: s2.at[n, ds8(((zi + k) % nz) * ZP, ZP)],
                     lambda k: r3.at[n, k - 1])

        def g3():
            arrived(9, got3)
            mine = ds8(zi * ZP, ZP)
            tot = s2[n, mine]
            for k in range(nz - 1):
                tot = tot + r3[n, k]
            t2[n, mine] = tot
            exchange(3, 10, z_peer, nz, lambda k: t2.at[n, mine], lambda k: t2.at[n, mine])

        def out_rows(k, h=0, size=piece):
            return ds8(base + ((me1 + k) % n1) * piece + h * half, size)

        def pass_on(rows, i, d):
            start([rcopy(dw_mine.at[rows], dw_mine.at[rows], *sems(3 if g == 2 else 5, i), sides[d])])

        def to_core(rows):
            start([rcopy(dw_mine.at[rows], dw_mine.at[rows], as_sem.at[n], cr_sem.at[n, 1], core_peer)])

        def g2():
            arrived(10, got3)
            rows = ds8(base + me1 * piece + me2 * sub, sub)
            exchange(4, 11, peer2, 4, lambda k: t2.at[n, top(sub)], lambda k: dw_mine.at[rows])
            dw_out[j, rows] = t2[n, top(sub)]

        def g1():
            arrived(11, got2)
            for i in range(4):
                pass_on(out_rows(0, (i + i // 2) % 2, half), 12 + min(i, 2), i % 2)
            to_core(out_rows(0))

        def g1m():
            for d, k in enumerate((3, 1)):
                rows = out_rows(k, d, half)
                arrived(12 + d, dw_mine.at[rows])
                pass_on(rows, 14, d)
                to_core(rows)

        def gather_end():
            arrived(14, r1.at[n, pl.ds(2, 4), top(half)])
            for k, h in ((3, 1), (1, 0)):
                to_core(out_rows(k, h, half))
            to_core(out_rows(2))

        def w0():
            arrived(9, got15)
            for d in DIRS:
                pass_on(out_rows(0), 12 + 4 * d, d)
            to_core(out_rows(0))

        def w_step(s):
            def step():
                for d in DIRS:
                    k = 8 - s if d == 0 else s
                    whole = out_rows(k)
                    arrived(12 + 4 * d + s - 1, dw_mine.at[whole])
                    pass_on(whole if s < 3 else out_rows(k, d, half), 12 + 4 * d + s, d)
                    to_core(whole)
            return step

        def w_end():
            for d in DIRS:
                arrived(15 + 4 * d, dw_mine.at[out_rows(4, d, half)])
            to_core(out_rows(4))

        def sent_all():
            middle = 2 * 15 * 8 if g == 2 else 6 * sub + 2 * (nz - 1) * ZP
            drain(as_sem.at[n], part.at[:, top((n1 - 1) * piece + (middle + own) // 2)])

        def finish():
            drain(cr_sem.at[n, 1], everything)
            drain(cs_sem.at[n], everything)

        steps = dict(cs=core_send, fin=finish, end=sent_all)
        if g == 2:
            steps.update(p1=z0, z1=z1, z2=z_step(2), z3=z_step(3), p2=z_end, p3=z_spread, g1=w0, w1=w_step(1),
                         w2=w_step(2), w3=w_step(3), gc=w_end)
        else:
            steps.update(p1=p1, p1m=p1m, p2=p2, p3=p3, g3=g3, g2=g2, g1=g1, g1m=g1m, gc=gather_end)
        return steps

    table = {}
    for i, c in enumerate("ABYabz"):
        g = i % 3
        table[c] = (g + (c == "Y"), int(c.isupper()), g, int(c not in "AB"))
    chains = {name: reducer(*spec[:3]) for name, spec in table.items()}

    def sums(*words):
        for word in words:
            names, step = word.split(".")
            for c in names:
                with scope(c + "_" + step):
                    chains[c][step]()

    def on_core(core, *words):
        @pl.when(ci == core)
        def _():
            sums(*words)

    def give(c):
        on_core(1 - table[c][3], c + ".cs")

    with scope("xlocal"):
        widen_local(xe, xc)
        conv_mid(xc, w1f, acc1)
    with scope("glocal"):
        widen_local(ge, gc)
        conv_mid(gc, w2t, acc2)
    greet(1)
    with scope("xrows"):
        recv_rows(0, xe)
    with scope("c1own"):
        widen_rows(xe, xc)
        conv_sides(xc, w1f, acc1)
    with scope("grows"):
        recv_rows(1, ge)
    with scope("ct2own"):
        widen_rows(ge, gc)
        conv_sides(gc, w2t, acc2)
    greet(2)
    for c in cw[3:soon]:
        c.wait()
    fetch(w1_hbm, w1r)
    fetch_own(w2_hbm, w2f)
    fetch_edge(w2_hbm, v2f)
    with scope("xplanes"):
        recv_planes(0, xe)
    with scope("c1rest"):
        widen_planes(xe, xc)
        conv_rest(xc, v1f, acc1, fin_a)
    greet(3)
    with scope("late"):
        for c in cw[soon:]:
            c.wait()
        flip(w1r, w1t, v1t)
    with scope("gplanes"):
        recv_planes(1, ge)
    with scope("gplanesw"):
        widen_planes(ge, gc)
    start_halo(2, ze, hz)
    for c in "YBA":
        with scope("d2"):
            wgrad(zt, gc, 1, table[c][2], True)
        give(c)
    with scope("ct2rest"):
        conv_rest(gc, v2t, acc2, fin_da)
    on_core(0, "B.p1")
    on_core(1, "Y.p1")
    with scope("d1z"):
        wgrad(at, xc, 0, 2, False)
    give("z")
    on_core(0, "A.p1")
    start_halo(3, ae, ha)
    with scope("d1b"):
        wgrad(at, xc, 0, 1, False)
    give("b")
    with scope("d1a"):
        wgrad(at, xc, 0, 0, False)
    give("a")
    on_core(1, "Y.z1", "z.p1")
    with scope("zhalo"):
        widen_local(ze, zc)
        recv_rows(2, ze)
        widen_rows(ze, zc)
    on_core(0, "B.p1m")
    on_core(1, "b.p1")
    with scope("c2own"):
        conv_own(zc, w2f, acc1)
    on_core(1, "a.p1", "z.z1")
    with scope("zplanes"):
        recv_planes(2, ze)
        widen_planes(ze, zc)
    on_core(1, "Y.z2")
    with scope("c2rest"):
        conv_rest(zc, v2f, acc1, fin_add(xe, y_out))
    on_core(0, "A.p1m")
    on_core(1, "b.p1m")
    with scope("ahalo"):
        widen_local(ae, ac)
        recv_rows(3, ae)
        widen_rows(ae, ac)
    on_core(0, "B.p2")
    with scope("ct1own"):
        conv_own(ac, w1t, acc2)
    on_core(1, "z.z2", "Y.z3", "a.p1m")
    with scope("aplanes"):
        recv_planes(3, ae)
        widen_planes(ae, ac)
    with scope("ct1rest"):
        conv_rest(ac, v1t, acc2, fin_add(ge, dx_out))
    on_core(0, "A.p2", "BA.p3", "BA.g3", "BA.g2", "BA.g1", "BA.g1m", "BA.gc")
    on_core(1, "b.p2", "z.z3", "Y.p2", "a.p2", "b.p3", "z.p2", "Y.p3", "a.p3", "z.p3", "b.g3", "Y.g1",
            "a.g3", "z.g1", "Y.w1", "b.g2", "a.g2", "z.w1", "Y.w2", "b.g1", "a.g1", "z.w2", "Y.w3",
            "ba.g1m", "z.w3", "Y.gc", "z.gc", "ba.gc")
    on_core(0, "Yzba.fin", "AB.end")
    on_core(1, "AB.fin", "Yzba.end")
    with scope("tail"):
        for sem, region in pending:
            drain(sem, region)


def settle(y, dx, dw, *refs):
    rows = top(ROWS)
    copies = [pltpu.make_async_copy(src, dst, refs[4].at[n])
              for n, (src, dst) in enumerate(zip((y, dx, dw.at[0, rows], dw.at[1, rows]), refs[:4]))]
    for c in copies:
        c.start()
    for c in copies:
        c.wait()


def solution(mesh):
    nrow, ndep = mesh.shape['row'], mesh.shape['dep']
    ny = 4 if nrow >= 16 else 2
    nx, nz = ndep // 2, nrow // ny
    vol = P(None, 'dep', 'row', None, None)

    def local_step(x, w1, w2, g):
        ext = (NB, ND + 2, NR + 2, NW, NC)
        wide = (NB, ND + 2, NR + 2, NW, 3 * NC)
        tile = (NB, ND, NR, NW, NC)
        V = pltpu.VMEM
        DMA = pltpu.SemaphoreType.DMA
        flops = 6 * 2 * NB * ND * NR * NW * ROWS * NC
        out = pl.pallas_call(
            functools.partial(kernel, nx, ny, nz),
            out_shape=(V((2048, NC), BF16),) * 2 + (V((2, ROWS, NC), F32),),
            in_specs=[pl.BlockSpec(memory_space=pl.ANY)] * 4,
            out_specs=(pl.BlockSpec(memory_space=V),) * 3,
            scratch_shapes=[V(ext, BF16)] * 4 + [V(wide, BF16)] * 4 + [V((ROWS, NC), BF16)] * 2
            + [V((2 * PLANE, 2 * NC), BF16)] * 4 + [V((2, 4 * TRIPLE, 2 * NC), BF16)] * 4
            + [V((NB, ND, NR * NW, NC), F32)] + [V((NC, 2048), BF16)] * 2
            + [V((4, 256, 256), F32)] * 2
            + [V((2, ROWS, NC), F32)] + [V((SLOTS, max(OWN), NC), F32)] * 2 + [
                V((SLOTS, 6, max(PIECE) // 2, NC), F32), V((SLOTS, 2, 4, PIECE[2], NC), F32),
                V((SLOTS, 3, max(SUB), NC), F32),
                V((SLOTS, 15, 8, NC), F32), V((SLOTS, nz - 1, ZP, NC), F32),
                V((SLOTS, max(PIECE), NC), F32), V((SLOTS, nz * ZP, NC), F32), V((SLOTS, nz * ZP, NC), F32),
                DMA((9,)), DMA((4,)), DMA((4, 2)), DMA((SLOTS,)), DMA((SLOTS, 2)),
                DMA((SLOTS,)), DMA((2, 15)), DMA((2, 20)), pltpu.SemaphoreType.REGULAR((3,))],
            compiler_params=pltpu.CompilerParams(
                collective_id=0, has_side_effects=True, vmem_limit_bytes=58720256),
            cost_estimate=pl.CostEstimate(flops=flops, bytes_accessed=8000000, transcendentals=0),
            name="resblock",
        )(x, w1.reshape(ROWS, NC), w2.reshape(ROWS, NC), g)
        shapes = [jax.ShapeDtypeStruct((n, NC), t) for n, t in ((2048, BF16), (ROWS, F32)) for _ in "ab"]
        y, dx, dw1, dw2 = pl.pallas_call(
            settle,
            out_shape=shapes,
            in_specs=[pl.BlockSpec(memory_space=V)] * 3,
            out_specs=[pl.BlockSpec(memory_space=pl.ANY)] * 4,
            scratch_shapes=[DMA((4,))],
            compiler_params=pltpu.CompilerParams(vmem_limit_bytes=1048576),
            cost_estimate=pl.CostEstimate(flops=0, bytes_accessed=8000000, transcendentals=0),
            name="settle",
        )(*out)
        return y.reshape(tile), dx.reshape(tile), dw1.reshape(w1.shape), dw2.reshape(w2.shape)

    return jax.shard_map(local_step, mesh=mesh, in_specs=(vol, P(), P(), vol),
                         out_specs=(vol, vol, P(), P()), check_vma=False)
```

```python
import functools

import jax
import jax.numpy as jnp
from jax import lax
from jax.experimental import pallas as pl
from jax.experimental.pallas import tpu as pltpu
from jax.sharding import PartitionSpec as P

MESH = pl.DeviceIdType.MESH
F32 = jnp.float32
BF16 = jnp.bfloat16

NB, ND, NR, NW, NC = 2, 2, 16, 32, 128
TAPS = 27
ROWS = TAPS * NC
FIRST = (0, 9, 19)
COUNT = (9, 10, 8)
RINGS = (4, 4, 8)
ZP = 16
BASE = tuple(t * NC for t in FIRST)
OWN = tuple(t * NC for t in COUNT)
PIECE = tuple(n // r for n, r in zip(OWN, RINGS))
SUB = tuple(n // 4 for n in PIECE)
DIRS = (0, 1)
SLOTS = 4
PLANE = 9 * NC
TRIPLE = 3 * NC
CHUNKS = ((0, 0), (0, 8), (1, 0), (1, 8))
NEIGH = ((1, 0), (-1, 0), (1, 1), (1, -1), (-1, 1), (-1, -1), (0, 1), (0, -1))


def top(n):
    return pl.ds(0, n)


def inner(n):
    return pl.ds(1, n)


def others(n):
    return range(1, n)


def kernel(nx, ny, nz, x_hbm, w1_hbm, w2_hbm, g_hbm,
           y_out, dx_out, dw_out,
           xe, ge, ze, ae, xc, gc, zc, ac,
           w1r, w2r, w1f, w2f, w1t, w2t, v1f, v2f, v1t, v2t, gp, zt, at,
           acc1, acc2, part, crecv, hsum, r1, rz, r2, r15, r3, s1, s2, t2,
           in_sem, hs_sem, hr_sem, cs_sem, cr_sem, as_sem, ar_sem, az_sem, greet_sem):
    row, dep = lax.axis_index("row"), lax.axis_index("dep")
    nrow, ndep = nz * ny, nx * 2
    zi, yi = row // ny, row % ny
    xi, ci = dep // 2, dep % 2

    def x_peer(k):
        return (row, ((xi + k) % nx) * 2 + ci)

    def y_peer(k):
        return (zi * ny + (yi + k) % ny, dep)

    def z_peer(k):
        return (((zi + k) % nz) * ny + yi, dep)

    core_peer = (row, xi * 2 + 1 - ci)

    def halo_peer(dr, dd):
        return ((row + dr + nrow) % nrow, (dep + dd + ndep) % ndep)

    cx = pltpu.make_async_copy(x_hbm, xe.at[:, inner(2), inner(NR)], in_sem.at[0])
    cg = pltpu.make_async_copy(g_hbm, ge.at[:, inner(2), inner(NR)], in_sem.at[1])
    cx.start()
    cg.start()

    def scope(name):
        return jax.named_scope(name)

    around = [peer(k) for peer, n in ((x_peer, nx), (y_peer, ny), (z_peer, nz)) for k in (1, n - 1)]
    partners = [halo_peer(a, b) for a, b in NEIGH] + around
    barrier = pltpu.get_barrier_semaphore()

    def signal(sem, peers):
        for p in peers:
            pl.semaphore_signal(sem, inc=1, device_id=p, device_id_type=MESH)

    signal(barrier, partners)
    cw = []

    def fetch(src, dst):
        c = pltpu.make_async_copy(src, dst, in_sem.at[2 + len(cw) % 7])
        c.start()
        cw.append(c)

    lanes = (top(NC), pl.ds(NC, NC))

    def fetch_own(w, full):
        for d in DIRS:
            fetch(w.at[pl.ds((1 - d) * PLANE, 2 * PLANE)], full.at[:, lanes[d]])

    def fetch_edge(w, edge):
        for p in DIRS:
            for r in DIRS:
                fetch(w.at[pl.ds(2 * p * PLANE, PLANE)], edge.at[p, pl.ds(r * TRIPLE, PLANE), lanes[r]])

    fetch_own(w1_hbm, w1f)
    fetch(w2_hbm, w2r)
    with scope("barrier"):
        pl.semaphore_wait(barrier, len(partners))

    def greet(i):
        if i:
            pl.semaphore_wait(greet_sem.at[i - 1], len(around))
        if i < 3:
            signal(greet_sem.at[i], around)

    def halo_copies(slot, ext):
        out = []
        for k, (dr, dd) in enumerate(NEIGH):
            se, de = {1: (pl.ds(2, 1), top(1)), -1: (inner(1), pl.ds(3, 1)),
                      0: (inner(2), inner(2))}[dd]
            sr, tr = {1: (pl.ds(NR, 1), top(1)), -1: (inner(1), pl.ds(NR + 1, 1)),
                      0: (inner(NR), inner(NR))}[dr]
            out.append(pltpu.make_async_remote_copy(
                src_ref=ext.at[:, se, sr], dst_ref=ext.at[:, de, tr],
                send_sem=hs_sem.at[slot], recv_sem=hr_sem.at[slot, min(k // 2, 1)],
                device_id=halo_peer(dr, dd), device_id_type=MESH))
        return out

    hx, hg, hz, ha = (halo_copies(i, e) for i, e in enumerate((xe, ge, ze, ae)))
    pending = []

    def start(copies):
        for c in copies:
            c.start()

    def drain(sem, region):
        pltpu.make_async_copy(region, region, sem).wait()

    def sent(sem, region):
        pending.append((sem, region))

    def start_halo(slot, ext, copies):
        start(copies)
        sent(hs_sem.at[slot], ext.at[:, :, top((2 * NR + 8) // 4)])

    def recv_rows(slot, ext):
        drain(hr_sem.at[slot, 0], ext.at[:, top(2), top(2)])

    def recv_planes(slot, ext):
        drain(hr_sem.at[slot, 1], ext.at[:, top(2)])

    cx.wait()
    start_halo(0, xe, hx)
    cg.wait()
    start_halo(1, ge, hg)

    greet(0)
    fetch_edge(w1_hbm, v1f)
    soon = len(cw)

    blank = jnp.zeros((TRIPLE, NC), BF16)
    for edge in (v1f, v2f, v1t, v2t):
        for p in DIRS:
            for r in DIRS:
                edge[p, pl.ds((1 - r) * PLANE, TRIPLE), lanes[r]] = blank
    for c in cw[:3]:
        c.wait()

    def flip(raw, out, edge):
        for u in range(TAPS):
            block = raw[pl.ds((TAPS - 1 - u) * NC, NC), :].T
            plane, at_row = u // 9, (u % 9) * NC
            for d in DIRS:
                if plane >= 1 - d and plane <= 2 - d:
                    out[pl.ds((plane - 1 + d) * PLANE + at_row, NC), lanes[d]] = block
            if plane != 1:
                for r in DIRS:
                    edge[plane // 2, pl.ds(r * TRIPLE + at_row, NC), lanes[r]] = block

    flip(w2r, w2t, v2t)

    def widen(vals, store):
        v = vals.astype(F32)
        col = lax.broadcasted_iota(jnp.int32, v.shape, 1)
        left = jnp.where(col == 0, 0.0, pltpu.roll(v, 1, 1))
        right = jnp.where(col == NW - 1, 0.0, pltpu.roll(v, NW - 1, 1))
        store(0, left.astype(BF16))
        store(1, vals)
        store(2, right.astype(BF16))

    def widen_part(ext, out, b, e, r0, nr, keep):
        vals = ext[b, e, pl.ds(r0, nr)]
        if keep is not None:
            vals = jnp.where(keep, vals, jnp.zeros_like(vals))

        def store(j, piece):
            out[b, e, pl.ds(r0, nr), :, pl.ds(j * NC, NC)] = piece

        widen(vals, store)

    def widen_local(ext, out):
        for b in range(NB):
            for e in (1, 2):
                for r0 in (1, 9):
                    widen_part(ext, out, b, e, r0, 8, None)

    edges = ((0, row > 0), (NR + 1, row < nrow - 1))

    def widen_rows(ext, out):
        for b in range(NB):
            for e in (1, 2):
                for r0, keep in edges:
                    widen_part(ext, out, b, e, r0, 1, keep)

    def widen_planes(ext, out):
        for b in range(NB):
            for e, ek in ((0, dep > 0), (3, dep < ndep - 1)):
                for r0, keep in edges:
                    widen_part(ext, out, b, e, r0, 1, jnp.logical_and(ek, keep))
                for r0 in (1, 9):
                    widen_part(ext, out, b, e, r0, 8, ek)

    def conv_own(src, wts, acc):
        for i, (b, r0) in enumerate(CHUNKS):
            acc[i] = conv_part(src, wts, range(3), r0, b)

    def conv_part(src, wts, drs, r0, b):
        lhs = jnp.concatenate([src[b, e, pl.ds(r0 + dr, 8)].reshape(8 * NW, 3 * NC)
                               for e in (1, 2) for dr in drs], axis=1)
        rhs = jnp.concatenate([wts[pl.ds(e * PLANE + dr * TRIPLE, TRIPLE), :]
                               for e in DIRS for dr in drs], axis=0)
        return jnp.dot(lhs, rhs, preferred_element_type=F32)

    def conv_mid(src, wts, acc):
        for i, (b, r0) in enumerate(CHUNKS):
            acc[i] = conv_part(src, wts, (1,), r0, b)

    def conv_sides(src, wts, acc):
        for i, (b, r0) in enumerate(CHUNKS):
            acc[i] = acc[i] + conv_part(src, wts, (0, 2), r0, b)

    def conv_rest(src, edge, acc, finish):
        for b in range(NB):
            for d in range(ND):
                lhs = jnp.concatenate(
                    [jnp.concatenate([src[b, 3 * d, 2 * i + k] for i in range(NR // 2)], axis=0)
                     for k in range(4)], axis=1)
                pairs = jnp.dot(lhs, edge[d], preferred_element_type=F32)
                for h in range(2):
                    some = pairs[h * NC:(h + 1) * NC]
                    rows = jnp.concatenate([some[:, r * NC:(r + 1) * NC].reshape(4, 1, NW, NC)
                                            for r in DIRS], axis=1).reshape(8 * NW, NC)
                    finish(b, d, 8 * h, acc[2 * b + h, :, lanes[d]] + rows)

    def put(ref, b, d, r0, vals):
        ref[b, d, pl.ds(r0, 8)] = vals.reshape(8, NW, NC)

    def fin_a(b, d, r0, acc):
        a = acc.astype(BF16).astype(F32)
        c0, c1 = 0.7978845608028654, 0.044715
        sq = a * a
        th_ = jnp.tanh(c0 * (a + c1 * (sq * a)))
        cdf = 0.5 * (1.0 + th_)
        z = (a * cdf).astype(BF16)
        slope = cdf + (0.5 * a) * (1.0 - th_ * th_) * (c0 * (1.0 + (3.0 * c1) * sq))
        gp[b, d, pl.ds(r0 * NW, 8 * NW)] = slope
        put(ze, b, d + 1, r0 + 1, z)
        zt[:, pl.ds((d * NB + b) * 512 + r0 * NW, 8 * NW)] = z.T

    def fin_da(b, d, r0, acc):
        da = (acc * gp[b, d, pl.ds(r0 * NW, 8 * NW)]).astype(BF16)
        put(ae, b, d + 1, r0 + 1, da)
        at[:, pl.ds((d * NB + b) * 512 + r0 * NW, 8 * NW)] = da.T

    def fin_add(base, out):
        def fin(b, d, r0, acc):
            res = base[b, d + 1, pl.ds(r0 + 1, 8)].reshape(8 * NW, NC).astype(F32)
            out[pl.ds((b * ND + d) * 512 + r0 * NW, 8 * NW), :] = (acc + res).astype(BF16)
        return fin

    def tap_rhs(src, u):
        ud, dr, dw = u // 9, (u // 3) % 3, u % 3
        return jnp.concatenate(
            [src[b, d + ud, pl.ds(dr, NR), :, pl.ds(dw * NC, NC)].reshape(NR * NW, NC)
             for d in range(ND) for b in range(NB)], axis=0)

    def wgrad(lhs_t, src, j, g, flipped):
        lhs = lhs_t[...]
        taps = [t for t in range(FIRST[g], FIRST[g] + COUNT[g]) if t < TAPS]
        for n in range(0, len(taps), 2):
            pair = taps[n:n + 2]
            rhs = jnp.concatenate(
                [tap_rhs(src, TAPS - 1 - t if flipped else t) for t in pair], axis=1)
            out = jnp.dot(lhs, rhs, preferred_element_type=F32)
            for m, t in enumerate(pair):
                block = out[:, m * NC:(m + 1) * NC]
                part[j, pl.ds(t * NC, NC), :] = block if flipped else block.T

    def rcopy(src, dst, ssem, rsem, peer):
        return pltpu.make_async_remote_copy(src_ref=src, dst_ref=dst, send_sem=ssem,
                                            recv_sem=rsem, device_id=peer, device_id_type=MESH)

    def ds8(base, size):
        return pl.ds(pl.multiple_of(base, 8), size)

    rings = ((x_peer, xi), (y_peer, yi), (z_peer, zi))

    def arrival(n, i):
        return (ar_sem if n < 2 else az_sem).at[n % 2, i]

    def reducer(n, j, g):
        own, piece, sub, n1 = OWN[g], PIECE[g], SUB[g], RINGS[g]
        half = piece // 2
        base = BASE[g]
        dw_mine = dw_out.at[j]
        (peer1, me1), (peer2, me2) = rings[g], rings[(1, 0, 0)[g]]
        sides = (peer1(1), peer1(n1 - 1))
        everything = crecv.at[n, top(own)]
        got2, got3, got15 = r2.at[n, :, top(sub)], r3.at[n], r15.at[n]

        def sems(phase, i):
            return as_sem.at[n], arrival(n, i)

        def arrived(i, region):
            drain(arrival(n, i), region)

        def exchange(phase, i, peers, n, src, dst):
            far_first = sorted(others(n), key=lambda k: -min(k, n - k))
            start([rcopy(src(k), dst(k), *sems(phase, i), peers(k)) for k in far_first])

        def core_send():
            start([rcopy(part.at[j, pl.ds(base, own)], everything,
                         cs_sem.at[n], cr_sem.at[n, 0], core_peer)])

        def rows_of(k, h):
            return ds8(((me1 + k) % n1) * piece + h * half, half)

        def rows_at(k):
            return ds8(((me1 + k) % n1) * piece, piece)

        def from_core():
            drain(cr_sem.at[n, 0], everything)
            for i in range(0, own, piece):
                hsum[n, pl.ds(i, piece)] = part[j, pl.ds(base + i, piece)] + crecv[n, pl.ds(i, piece)]

        def absorb(rows, more):
            hsum[n, rows] = hsum[n, rows] + more

        def ring_copy(i):
            k, h = ((2, 0), (2, 1), (1, 1), (3, 0), (1, 0), (3, 1))[i]
            return rcopy(hsum.at[n, rows_of(k, h)], r1.at[n, i, top(half)],
                         *sems(0, min(i, 2)), sides[i % 2])

        def p1():
            from_core()
            start([ring_copy(i) for i in range(4)])

        def p1m():
            for i, k in enumerate((1, 3)):
                arrived(i, r1.at[n, i, top(half)])
                absorb(rows_of(k, i), r1[n, i, top(half)])
                start([ring_copy(4 + i)])

        def flow(d, s):
            return (4 - s) if d == 0 else (4 + s)

        def z_copy(d, s, src, part_rows):
            start([rcopy(hsum.at[n, src], rz.at[n, d, s, part_rows], *sems(0, 4 * d + s), sides[d])])

        def part_of(h):
            return pl.ds(h * half, half)

        def z0():
            from_core()
            for d in DIRS:
                z_copy(d, 0, rows_of(4, d), part_of(d))
            for d in DIRS:
                z_copy(d, 1, rows_of(flow(d, 1), 1 - d), part_of(1 - d))

        def z1():
            for d in DIRS:
                arrived(4 * d, rz.at[n, d, 0, part_of(d)])
                rows = rows_of(flow(d, 1), d)
                absorb(rows, rz[n, d, 0, part_of(d)])
                z_copy(d, 1, rows, part_of(d))

        def z_step(s):
            def step():
                for d in DIRS:
                    arrived(4 * d + s - 1, rz.at[n, d, s - 1])
                    rows = rows_at(flow(d, s))
                    absorb(rows, rz[n, d, s - 1])
                    z_copy(d, s, rows, top(piece))
            return step

        def plane(phase, i, src, dst):
            for k in sorted(others(16), key=lambda k: -sum(min(q, nx - q) for q in divmod(k, nx))):
                px, py = (xi + k // nx) % nx, (yi + k % nx) % nx
                start([rcopy(src(px * 4 + py), dst(k - 1), *sems(phase, i), (zi * ny + py, px * 2 + ci))])

        def z_end():
            for d in DIRS:
                arrived(4 * d + 3, rz.at[n, d, 3])
            s1[n, top(piece)] = hsum[n, rows_at(0)] + rz[n, 0, 3] + rz[n, 1, 3]
            plane(1, 8, lambda q: s1.at[n, ds8(q * 8, 8)], lambda k: r15.at[n, k])

        def z_spread():
            arrived(8, got15)
            q = (xi * 4 + yi) * 8
            tot = s1[n, ds8(q, 8)]
            for k in range(15):
                tot = tot + r15[n, k]
            t2[n, top(8)] = tot
            rows = ds8(base + me1 * piece + q, 8)
            plane(2, 9, lambda q: t2.at[n, top(8)], lambda k: dw_mine.at[rows])
            dw_out[j, rows] = tot

        def p2():
            arrived(2, r1.at[n, pl.ds(2, 4), top(half)])
            for h, (u, v) in enumerate(((3, 4), (2, 5))):
                s1[n, part_of(h)] = hsum[n, rows_of(0, h)] + r1[n, u, top(half)] + r1[n, v, top(half)]
            exchange(1, 8, peer2, 4, lambda k: s1.at[n, ds8(((me2 + k) % nx) * sub, sub)],
                     lambda k: r2.at[n, k - 1, top(sub)])

        def p3():
            arrived(8, got2)
            tot = s1[n, ds8(me2 * sub, sub)]
            for k in range(3):
                tot = tot + r2[n, k, top(sub)]
            s2[n, top(sub)] = tot
            s2[n, pl.ds(sub, nz * ZP - sub)] = jnp.zeros((nz * ZP - sub, NC), F32)
            exchange(2, 9, z_peer, nz, lambda k: s2.at[n, ds8(((zi + k) % nz) * ZP, ZP)],
                     lambda k: r3.at[n, k - 1])

        def g3():
            arrived(9, got3)
            mine = ds8(zi * ZP, ZP)
            tot = s2[n, mine]
            for k in range(nz - 1):
                tot = tot + r3[n, k]
            t2[n, mine] = tot
            exchange(3, 10, z_peer, nz, lambda k: t2.at[n, mine], lambda k: t2.at[n, mine])

        def out_rows(k, h=0, size=piece):
            return ds8(base + ((me1 + k) % n1) * piece + h * half, size)

        def pass_on(rows, i, d):
            start([rcopy(dw_mine.at[rows], dw_mine.at[rows], *sems(3 if g == 2 else 5, i), sides[d])])

        def to_core(rows):
            start([rcopy(dw_mine.at[rows], dw_mine.at[rows], as_sem.at[n], cr_sem.at[n, 1], core_peer)])

        def g2():
            arrived(10, got3)
            rows = ds8(base + me1 * piece + me2 * sub, sub)
            exchange(4, 11, peer2, 4, lambda k: t2.at[n, top(sub)], lambda k: dw_mine.at[rows])
            dw_out[j, rows] = t2[n, top(sub)]

        def g1():
            arrived(11, got2)
            for i in range(4):
                pass_on(out_rows(0, (i + i // 2) % 2, half), 12 + min(i, 2), i % 2)
            to_core(out_rows(0))

        def g1m():
            for d, k in enumerate((3, 1)):
                rows = out_rows(k, d, half)
                arrived(12 + d, dw_mine.at[rows])
                pass_on(rows, 14, d)
                to_core(rows)

        def gather_end():
            arrived(14, r1.at[n, pl.ds(2, 4), top(half)])
            for k, h in ((3, 1), (1, 0)):
                to_core(out_rows(k, h, half))
            to_core(out_rows(2))

        def w0():
            arrived(9, got15)
            for d in DIRS:
                pass_on(out_rows(0), 12 + 4 * d, d)
            to_core(out_rows(0))

        def w_step(s):
            def step():
                for d in DIRS:
                    k = 8 - s if d == 0 else s
                    whole = out_rows(k)
                    arrived(12 + 4 * d + s - 1, dw_mine.at[whole])
                    pass_on(whole if s < 3 else out_rows(k, d, half), 12 + 4 * d + s, d)
                    to_core(whole)
            return step

        def w_end():
            for d in DIRS:
                arrived(15 + 4 * d, dw_mine.at[out_rows(4, d, half)])
            to_core(out_rows(4))

        def sent_all():
            middle = 2 * 15 * 8 if g == 2 else 6 * sub + 2 * (nz - 1) * ZP
            drain(as_sem.at[n], part.at[:, top((n1 - 1) * piece + (middle + own) // 2)])

        def finish():
            drain(cr_sem.at[n, 1], everything)
            drain(cs_sem.at[n], everything)

        steps = dict(cs=core_send, fin=finish, end=sent_all)
        if g == 2:
            steps.update(p1=z0, z1=z1, z2=z_step(2), z3=z_step(3), p2=z_end, p3=z_spread, g1=w0, w1=w_step(1),
                         w2=w_step(2), w3=w_step(3), gc=w_end)
        else:
            steps.update(p1=p1, p1m=p1m, p2=p2, p3=p3, g3=g3, g2=g2, g1=g1, g1m=g1m, gc=gather_end)
        return steps

    table = {}
    for i, c in enumerate("ABYabz"):
        g = i % 3
        table[c] = (g + (c == "Y"), int(c.isupper()), g, int(c not in "AB"))
    chains = {name: reducer(*spec[:3]) for name, spec in table.items()}

    def sums(*words):
        for word in words:
            names, step = word.split(".")
            for c in names:
                with scope(c + "_" + step):
                    chains[c][step]()

    def on_core(core, *words):
        @pl.when(ci == core)
        def _():
            sums(*words)

    def give(c):
        on_core(1 - table[c][3], c + ".cs")

    with scope("xlocal"):
        widen_local(xe, xc)
        conv_mid(xc, w1f, acc1)
    with scope("glocal"):
        widen_local(ge, gc)
        conv_mid(gc, w2t, acc2)
    greet(1)
    with scope("xrows"):
        recv_rows(0, xe)
    with scope("c1own"):
        widen_rows(xe, xc)
        conv_sides(xc, w1f, acc1)
    with scope("grows"):
        recv_rows(1, ge)
    with scope("ct2own"):
        widen_rows(ge, gc)
        conv_sides(gc, w2t, acc2)
    greet(2)
    for c in cw[3:soon]:
        c.wait()
    fetch(w1_hbm, w1r)
    fetch_own(w2_hbm, w2f)
    fetch_edge(w2_hbm, v2f)
    with scope("xplanes"):
        recv_planes(0, xe)
    with scope("c1rest"):
        widen_planes(xe, xc)
        conv_rest(xc, v1f, acc1, fin_a)
    greet(3)
    with scope("late"):
        for c in cw[soon:]:
            c.wait()
        flip(w1r, w1t, v1t)
    with scope("gplanes"):
        recv_planes(1, ge)
    with scope("gplanesw"):
        widen_planes(ge, gc)
    start_halo(2, ze, hz)
    for c in "YBA":
        with scope("d2"):
            wgrad(zt, gc, 1, table[c][2], True)
        give(c)
    with scope("ct2rest"):
        conv_rest(gc, v2t, acc2, fin_da)
    on_core(0, "B.p1")
    on_core(1, "Y.p1")
    with scope("d1z"):
        wgrad(at, xc, 0, 2, False)
    give("z")
    on_core(0, "A.p1")
    start_halo(3, ae, ha)
    with scope("d1b"):
        wgrad(at, xc, 0, 1, False)
    give("b")
    with scope("d1a"):
        wgrad(at, xc, 0, 0, False)
    give("a")
    on_core(1, "Y.z1", "z.p1")
    with scope("zhalo"):
        widen_local(ze, zc)
        recv_rows(2, ze)
        widen_rows(ze, zc)
    on_core(0, "B.p1m")
    on_core(1, "b.p1")
    with scope("c2own"):
        conv_own(zc, w2f, acc1)
    on_core(1, "a.p1", "z.z1")
    with scope("zplanes"):
        recv_planes(2, ze)
        widen_planes(ze, zc)
    on_core(1, "Y.z2")
    with scope("c2rest"):
        conv_rest(zc, v2f, acc1, fin_add(xe, y_out))
    on_core(0, "A.p1m")
    on_core(1, "b.p1m")
    with scope("ahalo"):
        widen_local(ae, ac)
        recv_rows(3, ae)
        widen_rows(ae, ac)
    on_core(0, "B.p2")
    with scope("ct1own"):
        conv_own(ac, w1t, acc2)
    on_core(1, "z.z2", "Y.z3", "a.p1m")
    with scope("aplanes"):
        recv_planes(3, ae)
        widen_planes(ae, ac)
    with scope("ct1rest"):
        conv_rest(ac, v1t, acc2, fin_add(ge, dx_out))
    on_core(0, "A.p2", "BA.p3", "BA.g3", "BA.g2", "BA.g1", "BA.g1m", "BA.gc")
    on_core(1, "b.p2", "z.z3", "Y.p2", "a.p2", "b.p3", "z.p2", "Y.p3", "a.p3", "z.p3", "b.g3", "Y.g1",
            "a.g3", "z.g1", "Y.w1", "b.g2", "a.g2", "z.w1", "Y.w2", "b.g1", "a.g1", "z.w2", "Y.w3",
            "ba.g1m", "z.w3", "Y.gc", "z.gc", "ba.gc")
    on_core(0, "Yzba.fin", "AB.end")
    on_core(1, "AB.fin", "Yzba.end")
    with scope("tail"):
        for sem, region in pending:
            drain(sem, region)


def settle(y, dx, dw, *refs):
    rows = top(ROWS)
    copies = [pltpu.make_async_copy(src, dst, refs[4].at[n])
              for n, (src, dst) in enumerate(zip((y, dx, dw.at[0, rows], dw.at[1, rows]), refs[:4]))]
    for c in reversed(copies):
        c.start()
    for c in copies:
        c.wait()


def solution(mesh):
    nrow, ndep = mesh.shape['row'], mesh.shape['dep']
    ny = 4 if nrow >= 16 else 2
    nx, nz = ndep // 2, nrow // ny
    vol = P(None, 'dep', 'row', None, None)

    def local_step(x, w1, w2, g):
        ext = (NB, ND + 2, NR + 2, NW, NC)
        wide = (NB, ND + 2, NR + 2, NW, 3 * NC)
        tile = (NB, ND, NR, NW, NC)
        V = pltpu.VMEM
        DMA = pltpu.SemaphoreType.DMA
        flops = 6 * 2 * NB * ND * NR * NW * ROWS * NC
        out = pl.pallas_call(
            functools.partial(kernel, nx, ny, nz),
            out_shape=(V((2048, NC), BF16),) * 2 + (V((2, ROWS, NC), F32),),
            in_specs=[pl.BlockSpec(memory_space=pl.ANY)] * 4,
            out_specs=(pl.BlockSpec(memory_space=V),) * 3,
            scratch_shapes=[V(ext, BF16)] * 4 + [V(wide, BF16)] * 4 + [V((ROWS, NC), BF16)] * 2
            + [V((2 * PLANE, 2 * NC), BF16)] * 4 + [V((2, 4 * TRIPLE, 2 * NC), BF16)] * 4
            + [V((NB, ND, NR * NW, NC), F32)] + [V((NC, 2048), BF16)] * 2
            + [V((4, 256, 256), F32)] * 2
            + [V((2, ROWS, NC), F32)] + [V((SLOTS, max(OWN), NC), F32)] * 2 + [
                V((SLOTS, 6, max(PIECE) // 2, NC), F32), V((SLOTS, 2, 4, PIECE[2], NC), F32),
                V((SLOTS, 3, max(SUB), NC), F32),
                V((SLOTS, 15, 8, NC), F32), V((SLOTS, nz - 1, ZP, NC), F32),
                V((SLOTS, max(PIECE), NC), F32), V((SLOTS, nz * ZP, NC), F32), V((SLOTS, nz * ZP, NC), F32),
                DMA((9,)), DMA((4,)), DMA((4, 2)), DMA((SLOTS,)), DMA((SLOTS, 2)),
                DMA((SLOTS,)), DMA((2, 15)), DMA((2, 20)), pltpu.SemaphoreType.REGULAR((3,))],
            compiler_params=pltpu.CompilerParams(
                collective_id=0, has_side_effects=True, vmem_limit_bytes=58720256),
            cost_estimate=pl.CostEstimate(flops=flops, bytes_accessed=8000000, transcendentals=0),
            name="resblock",
        )(x, w1.reshape(ROWS, NC), w2.reshape(ROWS, NC), g)
        shapes = [jax.ShapeDtypeStruct((n, NC), t) for n, t in ((2048, BF16), (ROWS, F32)) for _ in "ab"]
        y, dx, dw1, dw2 = pl.pallas_call(
            settle,
            out_shape=shapes,
            in_specs=[pl.BlockSpec(memory_space=V)] * 3,
            out_specs=[pl.BlockSpec(memory_space=pl.ANY)] * 4,
            scratch_shapes=[DMA((4,))],
            compiler_params=pltpu.CompilerParams(vmem_limit_bytes=1048576),
            cost_estimate=pl.CostEstimate(flops=0, bytes_accessed=8000000, transcendentals=0),
            name="settle",
        )(*out)
        return y.reshape(tile), dx.reshape(tile), dw1.reshape(w1.shape), dw2.reshape(w2.shape)

    return jax.shard_map(local_step, mesh=mesh, in_specs=(vol, P(), P(), vol),
                         out_specs=(vol, vol, P(), P()), check_vma=False)
```
